512 devices in a mesh: ctx: 128 (over y, z, core), tp: 4 (over x).
Axes of the slice: x: 4, y: 8, z: 8, core: 2. Of those that a mesh axis runs over, the one named last changes fastest.
Arguments:
- resid: bfloat16 [16384, 4096], P('ctx', 'tp'), may hold values from -6 to 6
- query: bfloat16 [16384, 4096], P('ctx', 'tp'), may hold values from -240 to 240
- key: bfloat16 [16384, 1024], P('ctx', 'tp'), may hold values from -8 to 8
- value: bfloat16 [16384, 1024], P('ctx', 'tp'), may hold values from -6 to 6
- router_logit: float32 [16384], P('ctx'), may hold values from -8 to 8
- norm_gain: bfloat16 [4096], P('tp'), may hold values from 0.099609375 to 1.8984375
- w_gate: bfloat16 [4096, 14336], P('tp', 'ctx'), may hold values from -0.09375 to 0.09375
- w_up: bfloat16 [4096, 14336], P('tp', 'ctx'), may hold values from -0.09375 to 0.09375
- w_down: bfloat16 [14336, 4096], P('ctx', 'tp'), may hold values from -0.046875 to 0.046875
- sel_index: int32 [128, 32], P('ctx'), may hold values from 0 to 127, as said below
- sel_count: int32 [128], P('ctx'), may hold values from 1 to 32, 2048 in all
Outputs:
- updated: bfloat16 [4096, 4096], P('ctx', 'tp')
The draws below stay inside these ranges and needn't reach their ends.
Inputs may be any that keep to these rules, and one draw needn't show every extreme that they name: `sel_index`: each row holds 32 distinct positions within one shard's 128 tokens; the first sel_count entries of row c are that shard's routed tokens, the rest are unused. `sel_count`: the counts sum to 2048; some shard holds exactly 32.
All inputs are finite; a program needn't handle non-finite values.
Results may differ from the reference program's by a relative error of at most 0.0044.
Values may be sent and summed in bfloat16 or wider, within the bound.
A program may use at most 64 MiB of HBM per device.

```python
import math
import jax
import jax.numpy as jnp
import numpy as np
from jax import lax

D = 4096
HEADS = 32
KV_HEADS = 8
HEAD_DIM = 128
FF = 14336
TOK_CTX = 128
CAP = 32
SEQ = 16384
SELECTED = 2048
N_CTX = 128


def drawn_rows(key):
    base = jax.random.fold_in(key, 11)
    first, second = jax.random.split(base, 2)
    keys = jax.random.normal(first, (SEQ, KV_HEADS * HEAD_DIM), jnp.float32)
    queries = jax.random.normal(second, (SEQ, HEADS * HEAD_DIM), jnp.float32)
    keys = jnp.clip(keys, -8.0, 8.0)
    return (keys, queries)


def draw_query(key, part):
    keys, queries = drawn_rows(key)
    return queries.astype(jnp.bfloat16)


def draw_key(key, part):
    keys, queries = drawn_rows(key)
    return keys.astype(jnp.bfloat16)


def draw_sel_index(key, part):
    base = jax.random.fold_in(key, 23)
    shard_keys = jax.random.split(base, N_CTX)

    def one_shard(shard_key):
        return jax.random.permutation(shard_key, TOK_CTX)[:CAP].astype(jnp.int32)
    return jax.vmap(one_shard)(shard_keys)


def level_of(key, extent, cuts, least, top_value):
    def one(dim, parts):
        draws = jax.random.uniform(jax.random.fold_in(jax.random.fold_in(key, 6), dim), (parts,), jnp.float32, least / len(cuts), top_value / len(cuts))
        return jnp.repeat(jnp.exp(draws), extent[dim] // parts).reshape((-1,) + (1,) * (len(extent) - dim - 1))

    gain = one(*cuts[0])
    for cut in cuts[1:]:
        gain = gain * one(*cut)
    return gain


def split_up(number_of, total, most, slope):
    loads = [(1 << 20) // math.isqrt(grade ** slope) + 1 for grade in range(2, number_of + 1)]
    surplus, given = total - most - (number_of - 1), [1] * (number_of - 1)
    while surplus > 0:
        candidates = [i for i in range(number_of - 1) if given[i] < most]
        mass, left = sum([loads[i] for i in candidates]), surplus
        for i in candidates:
            more = min(most - given[i], max(1, left * loads[i] // mass), surplus)
            given[i] = given[i] + more
            surplus = surplus - more
    return np.array([most] + given)


def ragged_sizes(key, number_of, total, most, skew):
    if number_of == 2:
        one = jax.random.randint(key, (), max(1, total - most), min(most, total - 1) + 1)
        return jnp.stack([one, total - one])
    lengths = jnp.asarray(split_up(number_of, total, most, skew), jnp.int32)
    couples = (number_of - 1) // 2
    giver, taker = lengths[1:1 + 2 * couples:2], lengths[2:2 + 2 * couples:2]
    room = jnp.minimum(giver - 1, most - taker)
    passed = jax.random.randint(jax.random.fold_in(key, 1), (couples,), 0, 1 << 20) % (room + 1)
    lengths = lengths.at[1:1 + 2 * couples:2].set(giver - passed).at[2:2 + 2 * couples:2].set(taker + passed)
    return lengths[jax.random.permutation(jax.random.fold_in(key, 2), number_of)]


def normal_values(key, shape, scale, limit, cuts=(), held_as=jnp.bfloat16):
    entries = scale * jax.random.normal(key, shape, jnp.float32)
    if cuts:
        entries = entries * level_of(key, shape, cuts, -0.22, 0.18)
    return jnp.clip(entries, -limit, limit).astype(held_as)


def setup_inputs(seed: int = 0) -> dict:
    streams_of = jax.random.split(jax.random.key(seed), 12)
    resid = normal_values(streams_of[0], (SEQ, D), 1.0, 6.0, ((0, 128), (1, 4)))
    query = draw_query(jax.random.fold_in(streams_of[11], 71), 0)
    key = draw_key(jax.random.fold_in(streams_of[11], 71), 0)
    value = normal_values(streams_of[3], (SEQ, KV_HEADS * HEAD_DIM), 1.0, 6.0, ((0, 128), (1, 4)))
    router_logit = normal_values(streams_of[4], (SEQ,), 2.0, 8.0, ((0, 128),), jnp.float32)
    norm_gain = jnp.clip(1.0 + 0.18 * jax.random.normal(streams_of[5], (D,), jnp.float32), 0.099609375, 1.8984375).astype(jnp.bfloat16)
    w_gate = normal_values(streams_of[6], (D, FF), D ** -0.5, 0.09375, ((0, 4), (1, 128)))
    w_up = normal_values(streams_of[7], (D, FF), D ** -0.5, 0.09375, ((0, 4), (1, 128)))
    w_down = normal_values(streams_of[8], (FF, D), FF ** -0.5, 0.046875, ((0, 128), (1, 4)))
    sel_index = draw_sel_index(jax.random.fold_in(streams_of[11], 71), 0)
    sel_count = ragged_sizes(streams_of[10], N_CTX, SELECTED, CAP, 1).astype(jnp.int32)
    return dict(resid=resid, query=query, key=key, value=value, router_logit=router_logit, norm_gain=norm_gain, w_gate=w_gate, w_up=w_up, w_down=w_down, sel_index=sel_index, sel_count=sel_count)


BIG_NEG = -1e+30
EPSILON = 1e-05

def reference(resid, query, key, value, router_logit, norm_gain, w_gate, w_up, w_down, sel_index, sel_count):
    slot = jnp.arange(CAP, dtype=jnp.int32)
    live = (slot[None, :] < sel_count[:, None]).reshape(-1)
    position = (jnp.arange(N_CTX, dtype=jnp.int32)[:, None] * TOK_CTX + sel_index).reshape(-1).astype(jnp.int32)
    key_pos = jnp.where(live, position, SEQ)
    rows_x = resid[position]
    slots = rows_x.shape[0]
    group = HEADS // KV_HEADS
    scale = HEAD_DIM ** (-0.5)
    q_heads = query[position].reshape(slots, HEADS, HEAD_DIM).transpose(1, 0, 2)
    k_heads = jnp.repeat(key[position].reshape(slots, KV_HEADS, HEAD_DIM).transpose(1, 0, 2), group, axis=0)
    v_heads = jnp.repeat(value[position].reshape(slots, KV_HEADS, HEAD_DIM).transpose(1, 0, 2), group, axis=0)
    allowed = key_pos[None, :] <= position[:, None]

    def one_head(operands):
        q_one, k_one, v_one = operands
        scores = jnp.dot(q_one, k_one.T, preferred_element_type=jnp.float32) * scale
        scores = jnp.where(allowed, scores, BIG_NEG)
        top = lax.optimization_barrier(jnp.max(scores, axis=1, keepdims=True))
        prob = jnp.exp(scores - top)
        total = lax.optimization_barrier(jnp.sum(prob, axis=1, keepdims=True))
        return jnp.dot(prob.astype(jnp.bfloat16), v_one, preferred_element_type=jnp.float32) / total
    head_out = lax.map(one_head, (q_heads, k_heads, v_heads))
    attn = head_out.transpose(1, 0, 2).reshape(slots, D)
    rows_float = rows_x.astype(jnp.float32)
    h_one = (rows_float + attn).astype(jnp.bfloat16)
    h_float = h_one.astype(jnp.float32)
    rscale = lax.rsqrt(lax.optimization_barrier(jnp.mean(h_float * h_float, axis=1)) + EPSILON)
    scaled = (h_float * norm_gain.astype(jnp.float32)[None, :]).astype(jnp.bfloat16)
    gate = rscale[:, None] * jnp.dot(scaled, w_gate, preferred_element_type=jnp.float32)
    up_val = rscale[:, None] * jnp.dot(scaled, w_up, preferred_element_type=jnp.float32)
    hidden = (jax.nn.silu(gate) * up_val).astype(jnp.bfloat16)
    mlp = jnp.dot(hidden, w_down, preferred_element_type=jnp.float32).astype(jnp.bfloat16)
    router = jax.nn.sigmoid(router_logit[position])
    result = rows_float + router[:, None] * (attn + mlp.astype(jnp.float32))
    return jnp.where(live[:, None], result, 0.0).astype(jnp.bfloat16)
```

```python
import functools

import jax
import jax.numpy as jnp
from jax import lax
from jax.experimental import pallas as pl
from jax.experimental.pallas import tpu as pltpu
from jax.sharding import Mesh
from jax.sharding import PartitionSpec as P

D = 4096
HEAD_DIM = 128
CAP = 32
RING = 8
TP = 4
NEG = -1e30
EPSILON = 1e-05
DEAD = 64.0
KEY_LIMIT = 8.0
CTX = ("cy", "cz", "cc")
MESH = pl.DeviceIdType.MESH
BF = jnp.bfloat16
F32 = jnp.float32
WAVES = 2


def dot(a, b):
    return jnp.dot(a, b, preferred_element_type=F32)


def dot_t(a, b):
    return lax.dot_general(a, b, (((1,), (1,)), ((), ())), preferred_element_type=F32)


def place():
    y, z = lax.axis_index("cy"), lax.axis_index("cz")
    core, x = lax.axis_index("cc"), lax.axis_index("tp")
    return y, z, core, x


def wrap(value):
    return lax.rem(value + RING, RING)


def first_axis(y, z, core, step):
    return {"cy": wrap(y + step * (1 - core)), "cz": wrap(z + step * core)}


def second_axis(y, z, core, step):
    return {"cy": wrap(y + step * core), "cz": wrap(z + step * (1 - core))}


def other_core(core):
    return {"cc": 1 - core}


def remote(src, dst, send, recv, device):
    return pltpu.make_async_remote_copy(
        src_ref=src, dst_ref=dst, send_sem=send, recv_sem=recv, device_id=device, device_id_type=MESH
    )


def greet(devices):
    barrier = pltpu.get_barrier_semaphore()
    for device in devices:
        pl.semaphore_signal(barrier, inc=1, device_id=device, device_id_type=MESH)
    pl.semaphore_wait(barrier, len(devices))


def attention_kernel(
    resid, query, key, value, logit, gain, idx_col, idx_row, count,
    attn_out, rows_out, x_out, gate_out,
    kv, q_ext, top, total, accum, squares,
    near_send, near_recv, far_send, far_recv, chip_send, chip_recv, sq_send, sq_recv,
):
    y, z, core, x = place()
    shard = y * 16 + z * 2 + core
    greet(
        [first_axis(y, z, core, d) for d in range(1, RING)]
        + [second_axis(y, z, core, 1), second_axis(y, z, core, RING - 1), other_core(core)]
        + [{"tp": lax.rem(x + d, TP)} for d in range(1, TP)]
    )
    width = resid.shape[1]
    kv_width = key.shape[1]
    heads = kv_width // HEAD_DIM
    group = width // kv_width
    index = idx_col[0:CAP, :]
    picks = index == lax.broadcasted_iota(jnp.int32, (CAP, resid.shape[0]), 1)
    onehot = jnp.where(picks, 1.0, 0.0).astype(BF)
    live = lax.broadcasted_iota(jnp.int32, (CAP, 1), 0) < count[0]
    keys = jnp.where(live, dot(onehot, key[...]), DEAD)
    kv[0, 0, 0, :, 0:kv_width] = keys.astype(BF)
    kv[0, 0, 0, :, kv_width : 2 * kv_width] = dot(onehot, value[...]).astype(BF)
    copies = []
    near = []
    for d in range(1, RING):
        near.append(
            remote(
                kv.at[0, 0, 0], kv.at[0, 0, d], near_send.at[d], near_recv.at[d],
                first_axis(y, z, core, d),
            )
        )
        near[-1].start()
    x_rows = dot(onehot, resid[...])
    x_out[...] = x_rows.astype(BF)
    q_rows = dot(onehot, query[...]).astype(BF)
    q_tall = group * CAP
    unit = jnp.where(lax.broadcasted_iota(jnp.int32, (16, HEAD_DIM), 1) == 0, 1.0, 0.0).astype(BF)
    for h in range(heads):
        for g in range(group):
            at = (h * group + g) * HEAD_DIM
            q_ext[h, g * CAP : (g + 1) * CAP, :] = q_rows[:, at : at + HEAD_DIM]
        q_ext[h, q_tall : q_tall + 16, :] = unit
    picked = jnp.sum(jnp.where(picks, logit[...], 0.0), axis=1, keepdims=True)
    gate_out[...] = jnp.broadcast_to(1.0 / (1.0 + jnp.exp(-picked)), gate_out.shape)
    top[...] = jnp.full(top.shape, NEG, F32)
    total[...] = jnp.zeros(total.shape, F32)
    accum[...] = jnp.zeros(accum.shape, F32)
    scale = HEAD_DIM ** (-0.5)
    block = RING * CAP
    lane = lax.broadcasted_iota(jnp.int32, (1, block), 1)

    def attend(slot, cls, own):
        kind = core + cls - 2 * core * cls
        mine1 = y * (1 - kind) + z * kind
        mine2 = z * (1 - kind) + y * kind
        from1 = jnp.bitwise_and(mine1 + RING - lax.shift_right_logical(lane, 5), RING - 1)
        from2 = wrap(mine2 - slot)
        source = (
            16 * (from1 * (1 - kind) + from2 * kind) + 2 * (from2 * (1 - kind) + from1 * kind) + kind
        )
        piece = kv[cls, slot].reshape(block, 2 * kv_width)
        for h in range(heads):
            k_part = piece[:, h * HEAD_DIM : (h + 1) * HEAD_DIM]
            v_part = piece[:, kv_width + h * HEAD_DIM : kv_width + (h + 1) * HEAD_DIM]
            both = dot_t(q_ext[h], k_part)
            alive = both[q_tall : q_tall + 1, :] <= KEY_LIMIT
            allowed = source < shard
            if own:
                same = jnp.logical_and(source == shard, idx_row[...] <= idx_col[...])
                allowed = jnp.logical_or(allowed, same)
            allowed = jnp.logical_and(allowed, alive)
            scores = jnp.where(allowed, both[0:q_tall, :] * scale, NEG)
            before = top[h]
            now = jnp.maximum(before, jnp.max(scores, axis=1, keepdims=True))
            prob = jnp.exp(scores - now)
            fade = jnp.exp(before - now)
            top[h] = now
            total[h] = total[h] * fade + jnp.sum(prob, axis=1, keepdims=True)
            accum[h] = accum[h] * fade + dot(prob.astype(BF), v_part)

    for copy in near:
        copy.wait_recv()
    copies += near
    part = RING // WAVES
    up = second_axis(y, z, core, 1)
    down = second_axis(y, z, core, RING - 1)

    def forward(way, step, wave):
        rows = pl.ds(wave * part, part)
        src = step - 1 if way == 0 else (RING - step + 1) % RING
        dst = step if way == 0 else RING - step
        return remote(
            kv.at[0, src, rows], kv.at[0, dst, rows],
            far_send.at[way, step, wave], far_recv.at[way, step, wave], up if way == 0 else down,
        )

    def across(slot, wave):
        rows = pl.ds(wave * part, part)
        return remote(
            kv.at[0, slot, rows], kv.at[1, slot, rows],
            chip_send.at[slot, wave], chip_recv.at[slot, wave], other_core(core),
        )

    steps = (RING // 2, RING // 2 - 1)
    started = {}

    def launch(way, step, wave):
        started[way, step, wave] = forward(way, step, wave)
        started[way, step, wave].start()

    shared = {}

    def share(slot, wave):
        shared[slot, wave] = across(slot, wave)
        shared[slot, wave].start()

    for wave in range(WAVES):
        for way in range(2):
            launch(way, 1, wave)
        share(0, wave)
    attend(0, 0, True)
    for step in range(1, RING // 2 + 1):
        for wave in range(WAVES):
            for way in range(2):
                if step <= steps[way]:
                    started[way, step, wave].wait_recv()
                    if step < steps[way]:
                        launch(way, step + 1, wave)
                    share(step if way == 0 else RING - step, wave)
        if step == 1:
            for wave in range(WAVES):
                shared[0, wave].wait_recv()
            attend(0, 1, False)
        else:
            last = step - 1
            for slot in (last, RING - last):
                for wave in range(WAVES):
                    shared[slot, wave].wait_recv()

            def one(i, carry, last=last):
                slot = jnp.where(i < 2, last, RING - last)
                attend(slot, lax.rem(i, 2), False)
                return carry

            lax.fori_loop(0, 4, one, 0)
    attend(RING // 2, 0, False)
    for wave in range(WAVES):
        shared[RING // 2, wave].wait_recv()
    attend(RING // 2, 1, False)
    copies += list(started.values()) + list(shared.values())

    for h in range(heads):
        mixed = accum[h] / total[h]
        for g in range(group):
            at = (h * group + g) * HEAD_DIM
            attn_out[:, at : at + HEAD_DIM] = mixed[g * CAP : (g + 1) * CAP, :]
    h_one = (x_rows + attn_out[...]).astype(BF).astype(F32)
    part_sum = jnp.sum(h_one * h_one, axis=1, keepdims=True)
    squares[0] = jnp.broadcast_to(part_sum, squares.shape[1:])
    sums = []
    for d in range(1, TP):
        sums.append(
            remote(squares.at[0], squares.at[d], sq_send.at[d], sq_recv.at[d], {"tp": lax.rem(x + d, TP)})
        )
        sums[-1].start()
    for copy in sums:
        copy.wait_recv()
    copies += sums
    whole = squares[0] + squares[1] + squares[2] + squares[3]
    rscale = lax.rsqrt(whole[:, 0:1] / D + EPSILON)
    rows_out[...] = (h_one * gain[...].astype(F32) * rscale).astype(BF)
    for copy in copies:
        copy.wait_send()


def mlp_kernel(
    members, blocks,
    h_ref, w_gate, w_up, w_down, x_ref, attn_ref, gate_ref, count,
    out_ref,
    rows, weight, down_w, part_sum, quarter, half_out, half_in, quarter_out, quarter_in, hidden,
    sum_out, sum_in, down_now, down_own, back_out, back_in,
    near_send, near_recv, far_send, far_recv, x_send, x_recv, sum_send, sum_recv,
    back_send, back_recv, w_send, w_recv,
):
    y, z, core, x = place()
    stride = RING // members
    whole = members * CAP
    half = whole // 2
    fourth = whole // 4
    hid = blocks * HEAD_DIM
    units = w_gate.shape[1]
    low, high = lax.rem(x, 2), lax.div(x, 2)
    odd = lax.rem(low + high, 2)
    flip = x + 1 - 2 * low
    mirror = TP - 1 - x
    first_x = {"tp": flip * (1 - core) + mirror * core}
    second_x = {"tp": mirror * (1 - core) + flip * core}
    keep_half = odd * (1 - core) + high * core
    keep_fourth = high * (1 - core) + low * core
    up = second_axis(y, z, core, 1)
    down = second_axis(y, z, core, RING - 1)
    greet(
        [first_axis(y, z, core, d * stride) for d in range(1, members)]
        + [up, down, other_core(core), first_x, second_x]
    )
    near = []
    for d in range(1, members):
        near.append(
            remote(
                h_ref, rows.at[0, pl.ds(d * CAP, CAP)], near_send.at[d], near_recv.at[d],
                first_axis(y, z, core, d * stride),
            )
        )
        near[-1].start()
    rows[0, 0:CAP, :] = h_ref[...]
    gates = pl.ds(0, HEAD_DIM)
    ups = pl.ds(hid, HEAD_DIM)
    weight[:, 0:HEAD_DIM] = jnp.zeros((weight.shape[0], HEAD_DIM), BF)
    weight[:, hid : hid + HEAD_DIM] = jnp.zeros((weight.shape[0], HEAD_DIM), BF)
    weight[:, 0:units] = w_gate[...]
    weight[:, hid : hid + units] = w_up[...]
    down_w[0:units, :] = w_down[...]
    down_w[units:HEAD_DIM, :] = jnp.zeros((HEAD_DIM - units, down_w.shape[1]), BF)
    shared = [
        remote(
            weight.at[:, gates], weight.at[:, pl.ds(HEAD_DIM, HEAD_DIM)], w_send.at[0], w_recv.at[0],
            other_core(core),
        ),
        remote(
            weight.at[:, ups], weight.at[:, pl.ds(hid + HEAD_DIM, HEAD_DIM)], w_send.at[1], w_recv.at[1],
            other_core(core),
        ),
        remote(
            down_w.at[pl.ds(0, HEAD_DIM)], down_w.at[pl.ds(HEAD_DIM, HEAD_DIM)], w_send.at[2],
            w_recv.at[2], other_core(core),
        ),
    ]
    for copy in shared:
        copy.start()

    def forward(way, step):
        span = pl.ds(way * half, half)
        return remote(
            rows.at[step - 1, span], rows.at[step, span], far_send.at[way, step], far_recv.at[way, step],
            up if way == 0 else down,
        )

    def sum_on(way, step):
        span = pl.ds(way * half, half)
        return remote(
            sum_out.at[step - 1, span], sum_in.at[step - 1, span],
            sum_send.at[way, step], sum_recv.at[way, step], up if way == 0 else down,
        )

    my_half = pl.multiple_of(keep_half * half, half)
    its_half = pl.multiple_of((1 - keep_half) * half, half)
    my_fourth = pl.multiple_of(keep_fourth * fourth, fourth)
    its_fourth = pl.multiple_of((1 - keep_fourth) * fourth, fourth)
    mine = pl.multiple_of(my_half + my_fourth, fourth)

    def x_one(t):
        return remote(half_out.at[t], half_in.at[t], x_send.at[0, t], x_recv.at[0, t], first_x)

    def x_two(t):
        return remote(quarter_out.at[t], quarter_in.at[t], x_send.at[1, t], x_recv.at[1, t], second_x)

    def x_three(t):
        span = pl.ds(mine, fourth)
        return remote(
            hidden.at[t, span], hidden.at[t, span], x_send.at[2, t], x_recv.at[2, t], second_x
        )

    def x_four(t):
        span = pl.ds(my_half, half)
        return remote(hidden.at[t, span], hidden.at[t, span], x_send.at[3, t], x_recv.at[3, t], first_x)

    def stage_a(t):
        @pl.when(t >= 1)
        def _():
            for way in range(2):
                forward(way, t).wait_recv()

        @pl.when(t < RING - 1)
        def _():
            for way in range(2):
                forward(way, t + 1).start()

        slot = lax.rem(t, 2)
        part_sum[slot] = dot(rows[t], weight[...])
        half_out[t] = part_sum[slot, pl.ds(its_half, half)].astype(BF)
        x_one(t).start()

    def stage_b(t):
        slot = lax.rem(t, 2)
        x_one(t).wait_recv()
        sent = part_sum[slot, pl.ds(pl.multiple_of(my_half + its_fourth, fourth), fourth)]
        quarter_out[t] = (sent + half_in[t, pl.ds(its_fourth, fourth)].astype(F32)).astype(BF)
        x_two(t).start()
        kept = part_sum[slot, pl.ds(mine, fourth)]
        quarter[slot] = kept + half_in[t, pl.ds(my_fourth, fourth)].astype(F32)

    def stage_c(t):
        slot = lax.rem(t, 2)
        x_two(t).wait_recv()
        both = quarter[slot] + quarter_in[t].astype(F32)
        gate, up_val = both[:, 0:hid], both[:, hid : 2 * hid]
        hidden[t, pl.ds(mine, fourth)] = (gate / (1.0 + jnp.exp(-gate)) * up_val).astype(BF)
        x_three(t).start()

    def stage_d(t):
        x_three(t).wait_recv()
        x_four(t).start()

    def stage_e(t):
        x_four(t).wait_recv()
        down_now[...] = dot(hidden[t], down_w[...])

        @pl.when(t == 0)
        def _():
            down_own[...] = down_now[...]

        @pl.when(t >= 2)
        def _():
            for way in range(2):
                sum_on(way, t - 1).wait_recv()
            down_now[...] += sum_in[t - 2].astype(F32)

        @pl.when(t >= 1)
        def _():
            sum_out[t - 1] = down_now[...].astype(BF)
            for way in range(2):
                sum_on(way, t).start()

    for copy in near + shared:
        copy.wait_recv()
    stages = (stage_a, stage_b, stage_c, stage_d, stage_e)

    def turn(t, carry):
        for lag in (0, 4, 3, 2, 1):
            @pl.when(jnp.logical_and(t >= lag, t < RING + lag))
            def _(lag=lag):
                stages[lag](t - lag)

        return carry

    lax.fori_loop(0, RING + 4, turn, 0)
    for way in range(2):
        sum_on(way, RING - 1).wait_recv()
    down_own[...] += sum_in[RING - 2].astype(F32)
    back_out[...] = down_own[...].astype(BF)
    back = []
    for d in range(1, members):
        back.append(
            remote(
                back_out.at[pl.ds(d * CAP, CAP)], back_in.at[d], back_send.at[d], back_recv.at[d],
                first_axis(y, z, core, RING - d * stride),
            )
        )
        back[-1].start()
    mlp = down_own[0:CAP, :]
    for d in range(1, members):
        back[d - 1].wait_recv()
        mlp = mlp + back_in[d].astype(F32)
    mlp = mlp.astype(BF).astype(F32)
    result = x_ref[...].astype(F32) + gate_ref[:, 0:1] * (attn_ref[...] + mlp)
    live = lax.broadcasted_iota(jnp.int32, (CAP, 1), 0) < count[0]
    out_ref[...] = jnp.where(live, result, 0.0).astype(BF)
    for copy in near + shared + back:
        copy.wait_send()

    def drain(t, carry):
        for copy in (x_one(t), x_two(t), x_three(t), x_four(t)):
            copy.wait_send()

        @pl.when(t >= 1)
        def _():
            for way in range(2):
                forward(way, t).wait_send()
                sum_on(way, t).wait_send()

        return carry

    lax.fori_loop(0, RING, drain, 0)


def vmem(count):
    return [pl.BlockSpec(memory_space=pltpu.VMEM)] * count


SCALAR = pl.BlockSpec(memory_space=pltpu.SMEM)
DMA = pltpu.SemaphoreType.DMA


def local(
    resid, query, key, value, router_logit, norm_gain, w_gate, w_up, w_down, sel_index, sel_count
):
    width = resid.shape[1]
    tall = width // key.shape[1] * CAP
    heads = key.shape[1] // HEAD_DIM
    block = RING * CAP
    idx_col = jnp.tile(sel_index[0], tall // CAP)[:, None]
    idx_row = jnp.pad(sel_index, ((0, 0), (0, block - CAP)))
    attn, rows, x_rows, gate = pl.pallas_call(
        attention_kernel,
        out_shape=[
            jax.ShapeDtypeStruct((CAP, width), F32),
            jax.ShapeDtypeStruct((CAP, width), BF),
            jax.ShapeDtypeStruct((CAP, width), BF),
            jax.ShapeDtypeStruct((CAP, HEAD_DIM), F32),
        ],
        in_specs=vmem(8) + [SCALAR],
        out_specs=vmem(4),
        scratch_shapes=[
            pltpu.VMEM((2, RING, RING, CAP, 2 * key.shape[1]), BF),
            pltpu.VMEM((heads, tall + 16, HEAD_DIM), BF),
            pltpu.VMEM((heads, tall, 1), F32),
            pltpu.VMEM((heads, tall, 1), F32),
            pltpu.VMEM((heads, tall, HEAD_DIM), F32),
            pltpu.VMEM((TP, CAP, HEAD_DIM), F32),
            DMA((RING,)), DMA((RING,)),
            DMA((2, RING, WAVES)), DMA((2, RING, WAVES)),
            DMA((RING, WAVES)), DMA((RING, WAVES)),
            DMA((TP,)), DMA((TP,)),
        ],
        compiler_params=pltpu.CompilerParams(collective_id=0, has_side_effects=True),
        name="attend",
    )(
        resid, query, key, value, router_logit[None, :], norm_gain[None, :], idx_col, idx_row, sel_count
    )
    members, blocks = 8, 2
    whole = members * CAP
    hid = blocks * HEAD_DIM
    return pl.pallas_call(
        functools.partial(mlp_kernel, members, blocks),
        out_shape=jax.ShapeDtypeStruct((CAP, width), BF),
        in_specs=vmem(7) + [SCALAR],
        out_specs=vmem(1)[0],
        scratch_shapes=[
            pltpu.VMEM((RING, whole, width), BF),
            pltpu.VMEM((width, 2 * hid), BF),
            pltpu.VMEM((hid, width), BF),
            pltpu.VMEM((2, whole, 2 * hid), F32),
            pltpu.VMEM((2, whole // 4, 2 * hid), F32),
            pltpu.VMEM((RING, whole // 2, 2 * hid), BF),
            pltpu.VMEM((RING, whole // 2, 2 * hid), BF),
            pltpu.VMEM((RING, whole // 4, 2 * hid), BF),
            pltpu.VMEM((RING, whole // 4, 2 * hid), BF),
            pltpu.VMEM((RING, whole, hid), BF),
            pltpu.VMEM((RING - 1, whole, width), BF),
            pltpu.VMEM((RING - 1, whole, width), BF),
            pltpu.VMEM((whole, width), F32),
            pltpu.VMEM((whole, width), F32),
            pltpu.VMEM((whole, width), BF),
            pltpu.VMEM((members, CAP, width), BF),
            DMA((RING,)), DMA((RING,)),
            DMA((2, RING)), DMA((2, RING)),
            DMA((4, RING)), DMA((4, RING)),
            DMA((2, RING)), DMA((2, RING)),
            DMA((RING,)), DMA((RING,)),
            DMA((3,)), DMA((3,)),
        ],
        compiler_params=pltpu.CompilerParams(collective_id=1, has_side_effects=True),
        name="mlp",
    )(rows, w_gate, w_up, w_down, x_rows, attn, gate, sel_count)


def solution(mesh):
    split = Mesh(mesh.devices.reshape(8, 8, 2, mesh.shape["tp"]), (*CTX, "tp"))
    placed = (
        P(CTX, "tp"),
        P(CTX, "tp"),
        P(CTX, "tp"),
        P(CTX, "tp"),
        P(CTX),
        P("tp"),
        P("tp", CTX),
        P("tp", CTX),
        P(CTX, "tp"),
        P(CTX, None),
        P(CTX),
    )
    return jax.shard_map(
        local, mesh=split, in_specs=placed, out_specs=P(CTX, "tp"), check_vma=False
    )
```

```python
import functools

import jax
import jax.numpy as jnp
from jax import lax
from jax.experimental import pallas as pl
from jax.experimental.pallas import tpu as pltpu
from jax.sharding import Mesh
from jax.sharding import PartitionSpec as P

D = 4096
HEAD_DIM = 128
CAP = 32
RING = 8
TP = 4
NEG = -1e30
EPSILON = 1e-05
DEAD = 64.0
KEY_LIMIT = 8.0
CTX = ("cy", "cz", "cc")
MESH = pl.DeviceIdType.MESH
BF = jnp.bfloat16
F32 = jnp.float32
SHARES = 2
ORDER = (0, 1, 7, 2, 6, 3, 5, 4)
MEMBERS = 4
BLOCKS = 4


def dot(a, b):
    return jnp.dot(a, b, preferred_element_type=F32)


def dot_t(a, b):
    return lax.dot_general(a, b, (((1,), (1,)), ((), ())), preferred_element_type=F32)


def place():
    y, z = lax.axis_index("cy"), lax.axis_index("cz")
    core, x = lax.axis_index("cc"), lax.axis_index("tp")
    return y, z, core, x


def wrap(value):
    return lax.rem(value + RING, RING)


def first_axis(y, z, core, step):
    return {"cy": wrap(y + step * (1 - core)), "cz": wrap(z + step * core)}


def second_axis(y, z, core, step):
    return {"cy": wrap(y + step * core), "cz": wrap(z + step * (1 - core))}


def other_core(core):
    return {"cc": 1 - core}


def remote(src, dst, send, recv, device):
    return pltpu.make_async_remote_copy(
        src_ref=src, dst_ref=dst, send_sem=send, recv_sem=recv, device_id=device, device_id_type=MESH
    )


def greet(devices):
    barrier = pltpu.get_barrier_semaphore()
    for device in devices:
        pl.semaphore_signal(barrier, inc=1, device_id=device, device_id_type=MESH)
    pl.semaphore_wait(barrier, len(devices))


def block_kernel(
    resid, query, key, value, logit, gain, picked_at, w_gate, w_up, w_down, count,
    out_ref,
    kv, q_ext, top, total, accum, squares, idx_wide, attn,
    gate_up, down_w, rows, scaled, part_sum, quarter, half_out, half_in, quarter_out, quarter_in,
    hidden, sum_out, sum_in, down_now, down_own, back_out, back_in,
    near_send, near_recv, far_send, far_recv, chip_send, chip_recv, sq_send, sq_recv,
    w_send, w_recv, row_send, row_recv, ring_send, ring_recv, x_send, x_recv, y_send, y_recv,
    sum_send, sum_recv, back_send, back_recv,
):
    y, z, core, x = place()
    shard = y * 16 + z * 2 + core
    odd1 = lax.rem(y * (1 - core) + z * core, 2)
    odd2 = lax.rem(z * (1 - core) + y * core, 2)
    twin = first_axis(y, z, core, 1 - 2 * odd1)
    cross = {**second_axis(y, z, core, 1 - 2 * odd2), "cc": 1 - core}
    cross_from = {**twin, "cc": 1 - core}
    up = second_axis(y, z, core, 1)
    down = second_axis(y, z, core, RING - 1)
    units = w_gate.shape[0]
    gate_up[0, 0] = w_gate[...]
    gate_up[1, 0] = w_up[...]
    down_w[0] = w_down[...]
    greet(
        [first_axis(y, z, core, d) for d in range(1, RING)]
        + [up, down, other_core(core), cross, cross_from]
        + [{"tp": lax.rem(x + d, TP)} for d in range(1, TP)]
    )
    width = resid.shape[1]
    kv_width = key.shape[1]
    heads = kv_width // HEAD_DIM
    group = width // kv_width
    row_f = picked_at[...].astype(F32)
    eye = lax.broadcasted_iota(jnp.int32, (CAP, CAP), 0) == lax.broadcasted_iota(
        jnp.int32, (CAP, CAP), 1
    )
    col_f = jnp.sum(jnp.where(eye, row_f, 0.0), axis=1, keepdims=True)
    spots = lax.broadcasted_iota(jnp.int32, (CAP, resid.shape[0]), 1).astype(F32)
    picks = col_f == spots
    onehot = jnp.where(picks, 1.0, 0.0).astype(BF)
    live = lax.broadcasted_iota(jnp.int32, (CAP, 1), 0) < count[0]
    keys = jnp.where(live, dot(onehot, key[...]), DEAD)
    kv[0, 0, 0, :, 0:kv_width] = keys.astype(BF)
    kv[0, 0, 0, :, kv_width : 2 * kv_width] = dot(onehot, value[...]).astype(BF)
    copies = []
    near = {}
    for d in (4, 3, 5, 2, 6, 1, 7):
        near[d] = remote(
            kv.at[0, 0, 0], kv.at[0, 0, d], near_send.at[d], near_recv.at[d],
            first_axis(y, z, core, d),
        )
        near[d].start()
    steps = (RING // 2, RING // 2 - 1)
    started = {}

    def launch(way, step, wave):
        src = step - 1 if way == 0 else (RING - step + 1) % RING
        dst = step if way == 0 else RING - step
        started[way, step, wave] = remote(
            kv.at[0, src, wave], kv.at[0, dst, wave],
            far_send.at[way, step, wave], far_recv.at[way, step, wave], up if way == 0 else down,
        )
        started[way, step, wave].start()

    shared = {}
    part = RING // SHARES

    def share(slot, piece):
        span = pl.ds(piece * part, part)
        shared[slot, piece] = remote(
            kv.at[0, slot, span], kv.at[1, slot, span],
            chip_send.at[slot, piece], chip_recv.at[slot, piece], other_core(core),
        )
        shared[slot, piece].start()

    for way in range(2):
        launch(way, 1, 0)
    across = [
        remote(
            gate_up.at[:, 0], gate_up.at[:, 1], w_send.at[0, 0], w_recv.at[0, 0], other_core(core)
        ),
        remote(down_w.at[0], down_w.at[1], w_send.at[1, 0], w_recv.at[1, 0], other_core(core)),
    ]
    for copy in across:
        copy.start()
    weight_span = 16
    pending = []
    for kind in range(2):
        for at in range(0, units, weight_span):
            for dest, device in ((2, twin), (3, cross)):
                pending.append((kind, at, dest, device))

    def send_weights(number):
        for kind, at, dest, device in pending[:number]:
            span = pl.ds(at, weight_span)
            if kind == 0:
                src, dst = gate_up.at[:, 0, span], gate_up.at[:, dest, span]
            else:
                src, dst = down_w.at[0, span], down_w.at[dest, span]
            remote(src, dst, w_send.at[kind, dest - 1], w_recv.at[kind, dest - 1], device).start()
        del pending[:number]

    def all_of(kind, dest):
        if kind == 0:
            src, dst = gate_up.at[:, 0], gate_up.at[:, dest]
        else:
            src, dst = down_w.at[0], down_w.at[dest]
        return remote(src, dst, w_send.at[kind, dest - 1], w_recv.at[kind, dest - 1], twin)

    x_rows = dot(onehot, resid[...])
    q_rows = dot(onehot, query[...]).astype(BF)
    q_tall = group * CAP
    unit = jnp.where(lax.broadcasted_iota(jnp.int32, (16, HEAD_DIM), 1) == 0, 1.0, 0.0).astype(BF)
    for h in range(heads):
        for g in range(group):
            at = (h * group + g) * HEAD_DIM
            q_ext[h, g * CAP : (g + 1) * CAP, :] = q_rows[:, at : at + HEAD_DIM]
        q_ext[h, q_tall : q_tall + 16, :] = unit
    chosen = jnp.sum(jnp.where(picks, logit[...], 0.0), axis=1, keepdims=True)
    router = 1.0 / (1.0 + jnp.exp(-chosen))
    idx_wide[...] = jnp.zeros(idx_wide.shape, F32)
    idx_wide[:, 0:CAP] = row_f
    idx_tall = jnp.concatenate([col_f] * group, axis=0)
    top[...] = jnp.full(top.shape, NEG, F32)
    total[...] = jnp.zeros(total.shape, F32)
    accum[...] = jnp.zeros(accum.shape, F32)
    scale = HEAD_DIM ** (-0.5)
    block = RING * CAP
    lane = lax.broadcasted_iota(jnp.int32, (1, block), 1)

    def attend(slot, cls, own):
        kind = core + cls - 2 * core * cls
        mine1 = y * (1 - kind) + z * kind
        mine2 = z * (1 - kind) + y * kind
        from1 = jnp.bitwise_and(mine1 + RING - lax.shift_right_logical(lane, 5), RING - 1)
        from2 = wrap(mine2 - slot)
        source = (
            16 * (from1 * (1 - kind) + from2 * kind) + 2 * (from2 * (1 - kind) + from1 * kind) + kind
        )
        piece = kv[cls, slot].reshape(block, 2 * kv_width)
        for h in range(heads):
            k_part = piece[:, h * HEAD_DIM : (h + 1) * HEAD_DIM]
            v_part = piece[:, kv_width + h * HEAD_DIM : kv_width + (h + 1) * HEAD_DIM]
            both = dot_t(q_ext[h], k_part)
            alive = both[q_tall : q_tall + 1, :] <= KEY_LIMIT
            allowed = source < shard
            if own:
                same = jnp.logical_and(source == shard, idx_wide[...] <= idx_tall)
                allowed = jnp.logical_or(allowed, same)
            allowed = jnp.logical_and(allowed, alive)
            scores = jnp.where(allowed, both[0:q_tall, :] * scale, NEG)
            before = top[h]
            now = jnp.maximum(before, jnp.max(scores, axis=1, keepdims=True))
            prob = jnp.exp(scores - now)
            fade = jnp.exp(before - now)
            top[h] = now
            total[h] = total[h] * fade + jnp.sum(prob, axis=1, keepdims=True)
            accum[h] = accum[h] * fade + dot(prob.astype(BF), v_part)

    for n, wave in enumerate(ORDER):
        if wave:
            near[wave].wait_recv()
            for way in range(2):
                launch(way, 1, wave)
        if wave == 3:
            share(0, 0)
    share(0, 1)
    send_weights(4)
    attend(0, 0, True)
    for step in range(1, RING // 2 + 1):
        for wave in ORDER:
            for way in range(2):
                if step <= steps[way]:
                    started[way, step, wave].wait_recv()
                    if step < steps[way]:
                        launch(way, step + 1, wave)
                    if wave in (3, 4):
                        share(step if way == 0 else RING - step, wave - 3)
        send_weights(4)
        if step == 1:
            for piece in range(SHARES):
                shared[0, piece].wait_recv()
            attend(0, 1, False)
        else:
            last = step - 1
            for slot in (last, RING - last):
                for piece in range(SHARES):
                    shared[slot, piece].wait_recv()

            def one(i, carry, last=last):
                slot = jnp.where(i < 2, last, RING - last)
                attend(slot, lax.rem(i, 2), False)
                return carry

            lax.fori_loop(0, 4, one, 0)
    attend(RING // 2, 0, False)
    for piece in range(SHARES):
        shared[RING // 2, piece].wait_recv()
    attend(RING // 2, 1, False)
    copies += list(near.values()) + list(started.values()) + list(shared.values()) + across
    for h in range(heads):
        mixed = accum[h] / total[h]
        for g in range(group):
            at = (h * group + g) * HEAD_DIM
            attn[:, at : at + HEAD_DIM] = mixed[g * CAP : (g + 1) * CAP, :]
    h_one = (x_rows + attn[...]).astype(BF).astype(F32)
    squares[0] = jnp.broadcast_to(jnp.sum(h_one * h_one, axis=1, keepdims=True), squares.shape[1:])
    sums = []
    for d in range(1, TP):
        sums.append(
            remote(squares.at[0], squares.at[d], sq_send.at[d], sq_recv.at[d], {"tp": lax.rem(x + d, TP)})
        )
        sums[-1].start()
    send_weights(4)
    for copy in sums:
        copy.wait_recv()
    copies += sums
    whole_sum = squares[0] + squares[1] + squares[2] + squares[3]
    rscale = lax.rsqrt(whole_sum[:, 0:1] / D + EPSILON)
    rows[0, 0:CAP, :] = (h_one * gain[...].astype(F32) * rscale).astype(BF)

    stride = RING // MEMBERS
    whole = MEMBERS * CAP
    half = whole // 2
    fourth = whole // 4
    hid = BLOCKS * units
    low, high = lax.rem(x, 2), lax.div(x, 2)
    odd = lax.rem(low + high, 2)
    flip = x + 1 - 2 * low
    mirror = TP - 1 - x
    first_x = {"tp": flip * (1 - core) + mirror * core}
    second_x = {"tp": mirror * (1 - core) + flip * core}
    keep_half = odd * (1 - core) + high * core
    keep_fourth = high * (1 - core) + low * core
    spread = []
    for d in range(1, MEMBERS):
        spread.append(
            remote(
                rows.at[0, pl.ds(0, CAP)], rows.at[0, pl.ds(d * CAP, CAP)],
                row_send.at[d], row_recv.at[d], first_axis(y, z, core, d * stride),
            )
        )
        spread[-1].start()

    def forward(member, step):
        span = pl.ds(member * CAP, CAP)
        return remote(
            rows.at[step - 1, span], rows.at[step, span], ring_send.at[member, step],
            ring_recv.at[member, step], up if member < MEMBERS // 2 else down,
        )

    def sum_on(member, step):
        span = pl.ds(member * CAP, CAP)
        return remote(
            sum_out.at[step - 1, span], sum_in.at[step - 1, span], sum_send.at[member, step],
            sum_recv.at[member, step], up if member < MEMBERS // 2 else down,
        )

    my_half = pl.multiple_of(keep_half * half, half)
    its_half = pl.multiple_of((1 - keep_half) * half, half)
    my_fourth = pl.multiple_of(keep_fourth * fourth, fourth)
    its_fourth = pl.multiple_of((1 - keep_fourth) * fourth, fourth)
    mine = pl.multiple_of(my_half + my_fourth, fourth)

    def x_one(t):
        return remote(half_out.at[t], half_in.at[t], x_send.at[0, t], x_recv.at[0, t], first_x)

    def x_two(t):
        return remote(quarter_out.at[t], quarter_in.at[t], x_send.at[1, t], x_recv.at[1, t], second_x)

    def x_hidden(d, t):
        span = pl.ds(mine, fourth)
        return remote(
            hidden.at[t, span], hidden.at[t, span], y_send.at[d, t], y_recv.at[d, t],
            {"tp": lax.rem(x + d, TP)},
        )

    def stage_a(t):
        for member in (0, 2, 1, 3):
            @pl.when(t >= 1)
            def _(member=member):
                forward(member, t).wait_recv()

            @pl.when(jnp.logical_and(t >= 1, t < RING - 1))
            def _(member=member):
                forward(member, t + 1).start()

        slot = lax.rem(t, 2)
        part_sum[slot] = dot_t(rows[t], gate_up[...].reshape(2 * hid, width))
        half_out[t] = part_sum[slot, pl.ds(its_half, half)].astype(BF)
        x_one(t).start()

    def stage_b(t):
        slot = lax.rem(t, 2)
        x_one(t).wait_recv()
        sent = part_sum[slot, pl.ds(pl.multiple_of(my_half + its_fourth, fourth), fourth)]
        quarter_out[t] = (sent + half_in[t, pl.ds(its_fourth, fourth)].astype(F32)).astype(BF)
        x_two(t).start()
        kept = part_sum[slot, pl.ds(mine, fourth)]
        quarter[slot] = kept + half_in[t, pl.ds(my_fourth, fourth)].astype(F32)

    def stage_c(t):
        slot = lax.rem(t, 2)
        x_two(t).wait_recv()
        both = quarter[slot] + quarter_in[t].astype(F32)
        gate, up_val = both[:, 0:hid], both[:, hid : 2 * hid]
        hidden[t, pl.ds(mine, fourth)] = (gate / (1.0 + jnp.exp(-gate)) * up_val).astype(BF)
        for d in (2, 1, 3):
            x_hidden(d, t).start()

    def stage_e(t):
        @pl.when(t == 0)
        def _():
            for dest in (2, 3):
                all_of(1, dest).wait_recv()

        for d in range(1, TP):
            x_hidden(d, t).wait_recv()
        down_now[...] = dot(hidden[t], down_w[...].reshape(hid, width))

        @pl.when(t == 0)
        def _():
            down_own[...] = down_now[...]

        for member in (0, 2, 1, 3):
            span = pl.ds(member * CAP, CAP)

            @pl.when(t >= 2)
            def _(member=member, span=span):
                sum_on(member, t - 1).wait_recv()
                down_now[span] += sum_in[t - 2, span].astype(F32)

            @pl.when(t >= 1)
            def _(member=member, span=span):
                sum_out[t - 1, span] = down_now[span].astype(BF)
                sum_on(member, t).start()

    forward(0, 1).start()
    send_weights(len(pending))
    for copy in across:
        copy.wait_recv()
    for d in (1, 3, 2):
        spread[d - 1].wait_recv()
        forward(d, 1).start()
    copies += spread
    for dest in (2, 3):
        all_of(0, dest).wait_recv()
    stages = (stage_a, stage_b, stage_c, stage_e)

    def turn(t, carry):
        for lag in (0, 3, 2, 1):
            @pl.when(jnp.logical_and(t >= lag, t < RING + lag))
            def _(lag=lag):
                stages[lag](t - lag)

        return carry

    lax.fori_loop(0, RING + 3, turn, 0)
    back = {}
    for member in (2, 3, 1, 0):
        span = pl.ds(member * CAP, CAP)
        sum_on(member, RING - 1).wait_recv()
        down_own[span] += sum_in[RING - 2, span].astype(F32)
        if member:
            back_out[span] = down_own[span].astype(BF)
            back[member] = remote(
                back_out.at[span], back_in.at[member], back_send.at[member], back_recv.at[member],
                first_axis(y, z, core, RING - member * stride),
            )
            back[member].start()
    mlp = down_own[0:CAP, :]
    for d in range(1, MEMBERS):
        back[d].wait_recv()
        mlp = mlp + back_in[d].astype(F32)
    mlp = mlp.astype(BF).astype(F32)
    result = x_rows + router * (attn[...] + mlp)
    out_ref[...] = jnp.where(live, result, 0.0).astype(BF)
    for copy in copies + list(back.values()):
        copy.wait_send()
    for kind in range(2):
        for dest in (2, 3):
            all_of(kind, dest).wait_send()

    def drain(t, carry):
        for copy in [x_one(t), x_two(t)] + [x_hidden(d, t) for d in range(1, TP)]:
            copy.wait_send()

        @pl.when(t >= 1)
        def _():
            for member in range(MEMBERS):
                forward(member, t).wait_send()
                sum_on(member, t).wait_send()

        return carry

    lax.fori_loop(0, RING, drain, 0)


def vmem(count):
    return [pl.BlockSpec(memory_space=pltpu.VMEM)] * count


SCALAR = pl.BlockSpec(memory_space=pltpu.SMEM)
DMA = pltpu.SemaphoreType.DMA


def local(
    resid, query, key, value, router_logit, norm_gain, w_gate, w_up, w_down, sel_index, sel_count
):
    width = resid.shape[1]
    tall = width // key.shape[1] * CAP
    heads = key.shape[1] // HEAD_DIM
    units = w_down.shape[0]
    whole = MEMBERS * CAP
    hid = BLOCKS * units
    return pl.pallas_call(
        block_kernel,
        out_shape=jax.ShapeDtypeStruct((CAP, width), BF),
        in_specs=vmem(10) + [SCALAR],
        out_specs=vmem(1)[0],
        scratch_shapes=[
            pltpu.VMEM((2, RING, RING, CAP, 2 * key.shape[1]), BF),
            pltpu.VMEM((heads, tall + 16, HEAD_DIM), BF),
            pltpu.VMEM((heads, tall, 1), F32),
            pltpu.VMEM((heads, tall, 1), F32),
            pltpu.VMEM((heads, tall, HEAD_DIM), F32),
            pltpu.VMEM((TP, CAP, HEAD_DIM), F32),
            pltpu.VMEM((1, RING * CAP), F32),
            pltpu.VMEM((CAP, width), F32),
            pltpu.VMEM((2, BLOCKS, units, width), BF),
            pltpu.VMEM((BLOCKS, units, width), BF),
            pltpu.VMEM((RING, whole, width), BF),
            pltpu.VMEM((CAP, width), BF),
            pltpu.VMEM((2, whole, 2 * hid), F32),
            pltpu.VMEM((2, whole // 4, 2 * hid), F32),
            pltpu.VMEM((RING, whole // 2, 2 * hid), BF),
            pltpu.VMEM((RING, whole // 2, 2 * hid), BF),
            pltpu.VMEM((RING, whole // 4, 2 * hid), BF),
            pltpu.VMEM((RING, whole // 4, 2 * hid), BF),
            pltpu.VMEM((RING, whole, hid), BF),
            pltpu.VMEM((RING - 1, whole, width), BF),
            pltpu.VMEM((RING - 1, whole, width), BF),
            pltpu.VMEM((whole, width), F32),
            pltpu.VMEM((whole, width), F32),
            pltpu.VMEM((whole, width), BF),
            pltpu.VMEM((MEMBERS, CAP, width), BF),
            DMA((RING,)), DMA((RING,)),
            DMA((2, RING // 2 + 1, RING)), DMA((2, RING // 2 + 1, RING)),
            DMA((RING, SHARES)), DMA((RING, SHARES)),
            DMA((TP,)), DMA((TP,)),
            DMA((2, 3)), DMA((2, 3)),
            DMA((MEMBERS,)), DMA((MEMBERS,)),
            DMA((MEMBERS, RING)), DMA((MEMBERS, RING)),
            DMA((2, RING)), DMA((2, RING)),
            DMA((TP, RING)), DMA((TP, RING)),
            DMA((MEMBERS, RING)), DMA((MEMBERS, RING)),
            DMA((MEMBERS,)), DMA((MEMBERS,)),
        ],
        compiler_params=pltpu.CompilerParams(collective_id=0, has_side_effects=True),
        name="block",
    )(
        resid, query, key, value, router_logit[None, :], norm_gain[None, :], sel_index,
        w_gate.T, w_up.T, w_down, sel_count,
    )


def solution(mesh):
    split = Mesh(mesh.devices.reshape(8, 8, 2, mesh.shape["tp"]), (*CTX, "tp"))
    placed = (
        P(CTX, "tp"),
        P(CTX, "tp"),
        P(CTX, "tp"),
        P(CTX, "tp"),
        P(CTX),
        P("tp"),
        P("tp", CTX),
        P("tp", CTX),
        P(CTX, "tp"),
        P(CTX, None),
        P(CTX),
    )
    return jax.shard_map(
        local, mesh=split, in_specs=placed, out_specs=P(CTX, "tp"), check_vma=False
    )
```

```python
import functools

import jax
import jax.numpy as jnp
from jax import lax
from jax.experimental import pallas as pl
from jax.experimental.pallas import tpu as pltpu
from jax.sharding import Mesh
from jax.sharding import PartitionSpec as P

D = 4096
HEAD_DIM = 128
CAP = 32
RING = 8
TP = 4
NEG = -1e30
EPSILON = 1e-05
DEAD = 64.0
KEY_LIMIT = 8.0
CTX = ("cy", "cz", "cc")
MESH = pl.DeviceIdType.MESH
BF = jnp.bfloat16
F32 = jnp.float32
SHARES = 2
ORDER = (0, 1, 7, 2, 6, 3, 5, 4)
MEMBERS = 4
PACE = 3
BLOCKS = 4


def dot(a, b):
    return jnp.dot(a, b, preferred_element_type=F32)


def dot_t(a, b):
    return lax.dot_general(a, b, (((1,), (1,)), ((), ())), preferred_element_type=F32)


def place():
    y, z = lax.axis_index("cy"), lax.axis_index("cz")
    core, x = lax.axis_index("cc"), lax.axis_index("tp")
    return y, z, core, x


def wrap(value):
    return lax.rem(value + RING, RING)


def first_axis(y, z, core, step):
    return {"cy": wrap(y + step * (1 - core)), "cz": wrap(z + step * core)}


def second_axis(y, z, core, step):
    return {"cy": wrap(y + step * core), "cz": wrap(z + step * (1 - core))}


def other_core(core):
    return {"cc": 1 - core}


def remote(src, dst, send, recv, device):
    return pltpu.make_async_remote_copy(
        src_ref=src, dst_ref=dst, send_sem=send, recv_sem=recv, device_id=device, device_id_type=MESH
    )


def greet(devices):
    barrier = pltpu.get_barrier_semaphore()
    for device in devices:
        pl.semaphore_signal(barrier, inc=1, device_id=device, device_id_type=MESH)
    return lambda: pl.semaphore_wait(barrier, len(devices))


def block_kernel(
    resid_hbm, query_hbm, key_hbm, value_hbm, logit_hbm, gain_hbm, picked_hbm, w_gate, w_up, w_down,
    count,
    out_ref,
    resid, query, key, value, logit, gain, picked_at, load_sem,
    kv, q_ext, top, total, accum, squares, idx_wide, attn,
    gate_up, down_w, rows, part_sum, quarter, half_out, half_in, quarter_out, quarter_in,
    hidden, sum_out, sum_in, down_now, down_own, back_out, back_in,
    near_send, near_recv, far_send, far_recv, chip_send, chip_recv, sq_send, sq_recv,
    w_send, w_recv, row_send, row_recv, ring_send, ring_recv, x_send, x_recv, y_send, y_recv,
    sum_send, sum_recv, back_send, back_recv,
):
    y, z, core, x = place()
    shard = y * 16 + z * 2 + core
    odd1 = lax.rem(y * (1 - core) + z * core, 2)
    odd2 = lax.rem(z * (1 - core) + y * core, 2)
    twin = first_axis(y, z, core, 1 - 2 * odd1)
    cross = {**second_axis(y, z, core, 1 - 2 * odd2), "cc": 1 - core}
    cross_from = {**twin, "cc": 1 - core}
    up = second_axis(y, z, core, 1)
    down = second_axis(y, z, core, RING - 1)
    units = w_gate.shape[0]
    loads = []
    for n, (src, dst) in enumerate(
        (
            (picked_hbm, picked_at), (key_hbm, key), (value_hbm, value), (resid_hbm, resid),
            (query_hbm, query), (logit_hbm, logit), (gain_hbm, gain), (w_gate, gate_up.at[0, 0]),
            (w_up, gate_up.at[1, 0]), (w_down, down_w.at[0]),
        )
    ):
        loads.append(pltpu.make_async_copy(src, dst, load_sem.at[n]))
        loads[-1].start()
    entered = greet(
        [first_axis(y, z, core, d) for d in range(1, RING)]
        + [up, down, other_core(core), cross, cross_from]
        + [{"tp": lax.rem(x + d, TP)} for d in range(1, TP)]
    )
    for load in loads[0:3]:
        load.wait()
    width = resid.shape[1]
    kv_width = key.shape[1]
    heads = kv_width // HEAD_DIM
    group = width // kv_width
    row_f = picked_at[...].astype(F32)
    eye = lax.broadcasted_iota(jnp.int32, (CAP, CAP), 0) == lax.broadcasted_iota(
        jnp.int32, (CAP, CAP), 1
    )
    col_f = jnp.sum(jnp.where(eye, row_f, 0.0), axis=1, keepdims=True)
    spots = lax.broadcasted_iota(jnp.int32, (CAP, resid.shape[0]), 1).astype(F32)
    picks = col_f == spots
    onehot = jnp.where(picks, 1.0, 0.0).astype(BF)
    live = lax.broadcasted_iota(jnp.int32, (CAP, 1), 0) < count[0]
    keys = jnp.where(live, dot(onehot, key[...]), DEAD)
    kv[0, 0, 0, :, 0:kv_width] = keys.astype(BF)
    kv[0, 0, 0, :, kv_width : 2 * kv_width] = dot(onehot, value[...]).astype(BF)
    entered()
    copies = []
    near = {}
    for d in (4, 3, 5, 2, 6, 1, 7):
        near[d] = remote(
            kv.at[0, 0, 0], kv.at[0, 0, d], near_send.at[d], near_recv.at[d],
            first_axis(y, z, core, d),
        )
        near[d].start()
    steps = (RING // 2, RING // 2 - 1)
    started = {}

    def launch(way, step, wave):
        src = step - 1 if way == 0 else (RING - step + 1) % RING
        dst = step if way == 0 else RING - step
        started[way, step, wave] = remote(
            kv.at[0, src, wave], kv.at[0, dst, wave],
            far_send.at[way, step, wave], far_recv.at[way, step, wave], up if way == 0 else down,
        )
        started[way, step, wave].start()

    shared = {}
    part = RING // SHARES

    def share(slot, piece):
        span = pl.ds(piece * part, part)
        shared[slot, piece] = remote(
            kv.at[0, slot, span], kv.at[1, slot, span],
            chip_send.at[slot, piece], chip_recv.at[slot, piece], other_core(core),
        )
        shared[slot, piece].start()

    for way in range(2):
        launch(way, 1, 0)
    for load in loads[3:]:
        load.wait()
    across = [
        remote(
            gate_up.at[:, 0], gate_up.at[:, 1], w_send.at[0, 0], w_recv.at[0, 0], other_core(core)
        ),
        remote(down_w.at[0], down_w.at[1], w_send.at[1, 0], w_recv.at[1, 0], other_core(core)),
    ]
    for copy in across:
        copy.start()
    weight_span = 16
    pending = []
    for kind in range(2):
        for at in range(0, units, weight_span):
            for dest, device in ((2, twin), (3, cross)):
                pending.append((kind, at, dest, device))

    def send_weights(number):
        for kind, at, dest, device in pending[:number]:
            span = pl.ds(at, weight_span)
            if kind == 0:
                src, dst = gate_up.at[:, 0, span], gate_up.at[:, dest, span]
            else:
                src, dst = down_w.at[0, span], down_w.at[dest, span]
            remote(src, dst, w_send.at[kind, dest - 1], w_recv.at[kind, dest - 1], device).start()
        del pending[:number]

    def all_of(kind, dest):
        if kind == 0:
            src, dst = gate_up.at[:, 0], gate_up.at[:, dest]
        else:
            src, dst = down_w.at[0], down_w.at[dest]
        return remote(src, dst, w_send.at[kind, dest - 1], w_recv.at[kind, dest - 1], twin)

    x_rows = dot(onehot, resid[...])
    q_rows = dot(onehot, query[...]).astype(BF)
    q_tall = group * CAP
    unit = jnp.where(lax.broadcasted_iota(jnp.int32, (16, HEAD_DIM), 1) == 0, 1.0, 0.0).astype(BF)
    for h in range(heads):
        for g in range(group):
            at = (h * group + g) * HEAD_DIM
            q_ext[h, g * CAP : (g + 1) * CAP, :] = q_rows[:, at : at + HEAD_DIM]
        q_ext[h, q_tall : q_tall + 16, :] = unit
    chosen = jnp.sum(jnp.where(picks, logit[...], 0.0), axis=1, keepdims=True)
    router = 1.0 / (1.0 + jnp.exp(-chosen))
    idx_wide[...] = jnp.zeros(idx_wide.shape, F32)
    idx_wide[:, 0:CAP] = row_f
    idx_tall = jnp.concatenate([col_f] * group, axis=0)
    top[...] = jnp.full(top.shape, NEG, F32)
    total[...] = jnp.zeros(total.shape, F32)
    accum[...] = jnp.zeros(accum.shape, F32)
    scale = HEAD_DIM ** (-0.5)
    block = RING * CAP
    lane = lax.broadcasted_iota(jnp.int32, (1, block), 1)

    def attend(slot, cls, own):
        kind = core + cls - 2 * core * cls
        mine1 = y * (1 - kind) + z * kind
        mine2 = z * (1 - kind) + y * kind
        from1 = jnp.bitwise_and(mine1 + RING - lax.shift_right_logical(lane, 5), RING - 1)
        from2 = wrap(mine2 - slot)
        source = (
            16 * (from1 * (1 - kind) + from2 * kind) + 2 * (from2 * (1 - kind) + from1 * kind) + kind
        )
        piece = kv[cls, slot].reshape(block, 2 * kv_width)
        for h in range(heads):
            k_part = piece[:, h * HEAD_DIM : (h + 1) * HEAD_DIM]
            v_part = piece[:, kv_width + h * HEAD_DIM : kv_width + (h + 1) * HEAD_DIM]
            both = dot_t(q_ext[h], k_part)
            alive = both[q_tall : q_tall + 1, :] <= KEY_LIMIT
            allowed = source < shard
            if own:
                same = jnp.logical_and(source == shard, idx_wide[...] <= idx_tall)
                allowed = jnp.logical_or(allowed, same)
            allowed = jnp.logical_and(allowed, alive)
            scores = jnp.where(allowed, both[0:q_tall, :] * scale, NEG)
            before = top[h]
            now = jnp.maximum(before, jnp.max(scores, axis=1, keepdims=True))
            prob = jnp.exp(scores - now)
            fade = jnp.exp(before - now)
            top[h] = now
            total[h] = total[h] * fade + jnp.sum(prob, axis=1, keepdims=True)
            accum[h] = accum[h] * fade + dot(prob.astype(BF), v_part)

    for wave in ORDER:
        if wave:
            near[wave].wait_recv()
            for way in range(2):
                launch(way, 1, wave)
        if wave == 3:
            share(0, 0)
    share(0, 1)
    todo = [(0, 0), (0, 1)]

    def attend_next():
        slot, cls = todo.pop(0)
        if cls:
            for piece in range(SHARES):
                shared[slot, piece].wait_recv()
        attend(slot, cls, (slot, cls) == (0, 0))

    for step in range(1, RING // 2 + 1):
        for n, wave in enumerate(ORDER):
            for way in range(2):
                if step <= steps[way]:
                    started[way, step, wave].wait_recv()
                    if step < steps[way]:
                        launch(way, step + 1, wave)
                    if wave in (3, 4):
                        share(step if way == 0 else RING - step, wave - 3)
            if n % 2 and todo:
                attend_next()
        todo += [(step, 0), (RING - step, 0), (step, 1), (RING - step, 1)] if step < 4 else []
        send_weights(PACE)
    attend(RING // 2, 0, False)
    for piece in range(SHARES):
        shared[RING // 2, piece].wait_recv()
    attend(RING // 2, 1, False)
    copies += list(near.values()) + list(started.values()) + list(shared.values()) + across
    for h in range(heads):
        mixed = accum[h] / total[h]
        for g in range(group):
            at = (h * group + g) * HEAD_DIM
            attn[:, at : at + HEAD_DIM] = mixed[g * CAP : (g + 1) * CAP, :]
    h_one = (x_rows + attn[...]).astype(BF).astype(F32)
    squares[0] = jnp.broadcast_to(jnp.sum(h_one * h_one, axis=1, keepdims=True), squares.shape[1:])
    sums = []
    for d in range(1, TP):
        sums.append(
            remote(squares.at[0], squares.at[d], sq_send.at[d], sq_recv.at[d], {"tp": lax.rem(x + d, TP)})
        )
        sums[-1].start()
    send_weights(8)
    for copy in sums:
        copy.wait_recv()
    copies += sums
    whole_sum = squares[0] + squares[1] + squares[2] + squares[3]
    rscale = lax.rsqrt(whole_sum[:, 0:1] / D + EPSILON)
    rows[0, 0:CAP, :] = (h_one * gain[...].astype(F32) * rscale).astype(BF)

    stride = RING // MEMBERS
    whole = MEMBERS * CAP
    half = whole // 2
    fourth = whole // 4
    hid = BLOCKS * units
    low, high = lax.rem(x, 2), lax.div(x, 2)
    odd = lax.rem(low + high, 2)
    flip = x + 1 - 2 * low
    mirror = TP - 1 - x
    first_x = {"tp": flip * (1 - core) + mirror * core}
    second_x = {"tp": mirror * (1 - core) + flip * core}
    keep_half = odd * (1 - core) + high * core
    keep_fourth = high * (1 - core) + low * core
    spread = []
    for d in range(1, MEMBERS):
        spread.append(
            remote(
                rows.at[0, pl.ds(0, CAP)], rows.at[0, pl.ds(d * CAP, CAP)],
                row_send.at[d], row_recv.at[d], first_axis(y, z, core, d * stride),
            )
        )
    for d in (2, 1, 3):
        spread[d - 1].start()

    def forward(member, step):
        span = pl.ds(member * CAP, CAP)
        return remote(
            rows.at[step - 1, span], rows.at[step, span], ring_send.at[member, step],
            ring_recv.at[member, step], up if member < MEMBERS // 2 else down,
        )

    def sum_on(member, step):
        span = pl.ds(member * CAP, CAP)
        return remote(
            sum_out.at[step - 1, span], sum_in.at[step - 1, span], sum_send.at[member, step],
            sum_recv.at[member, step], up if member < MEMBERS // 2 else down,
        )

    my_half = pl.multiple_of(keep_half * half, half)
    its_half = pl.multiple_of((1 - keep_half) * half, half)
    my_fourth = pl.multiple_of(keep_fourth * fourth, fourth)
    its_fourth = pl.multiple_of((1 - keep_fourth) * fourth, fourth)
    mine = pl.multiple_of(my_half + my_fourth, fourth)

    def x_one(t):
        return remote(half_out.at[t], half_in.at[t], x_send.at[0, t], x_recv.at[0, t], first_x)

    def x_two(t):
        return remote(quarter_out.at[t], quarter_in.at[t], x_send.at[1, t], x_recv.at[1, t], second_x)

    def x_hidden(d, t):
        span = pl.ds(mine, fourth)
        return remote(
            hidden.at[t, span], hidden.at[t, span], y_send.at[d, t], y_recv.at[d, t],
            {"tp": lax.rem(x + d, TP)},
        )

    def stage_a(t):
        for member in (0, 2, 1, 3):
            @pl.when(t < RING - 1)
            def _(member=member):
                forward(member, t + 1).wait_recv()

            @pl.when(t < RING - 2)
            def _(member=member):
                forward(member, t + 2).start()

        @pl.when(t == 0)
        def _():
            for dest in (2, 3):
                all_of(0, dest).wait_recv()

        slot = lax.rem(t, 2)
        part_sum[slot] = dot_t(rows[lax.rem(t + 1, RING)], gate_up[...].reshape(2 * hid, width))
        half_out[t] = part_sum[slot, pl.ds(its_half, half)].astype(BF)
        x_one(t).start()

    def stage_b(t):
        slot = lax.rem(t, 2)
        x_one(t).wait_recv()
        sent = part_sum[slot, pl.ds(pl.multiple_of(my_half + its_fourth, fourth), fourth)]
        quarter_out[t] = (sent + half_in[t, pl.ds(its_fourth, fourth)].astype(F32)).astype(BF)
        x_two(t).start()
        kept = part_sum[slot, pl.ds(mine, fourth)]
        quarter[slot] = kept + half_in[t, pl.ds(my_fourth, fourth)].astype(F32)

    def stage_c(t):
        slot = lax.rem(t, 2)
        x_two(t).wait_recv()
        both = quarter[slot] + quarter_in[t].astype(F32)
        gate, up_val = both[:, 0:hid], both[:, hid : 2 * hid]
        hidden[t, pl.ds(mine, fourth)] = (gate / (1.0 + jnp.exp(-gate)) * up_val).astype(BF)
        for d in (2, 1, 3):
            x_hidden(d, t).start()

    def stage_e(t):
        @pl.when(t == 0)
        def _():
            for dest in (2, 3):
                all_of(1, dest).wait_recv()

        for d in range(1, TP):
            x_hidden(d, t).wait_recv()
        down_now[...] = dot(hidden[t], down_w[...].reshape(hid, width))

        @pl.when(t == RING - 1)
        def _():
            down_own[...] = down_now[...]

        for member in (0, 2, 1, 3):
            span = pl.ds(member * CAP, CAP)

            @pl.when(jnp.logical_and(t >= 1, t < RING - 1))
            def _(member=member, span=span):
                sum_on(member, t).wait_recv()
                down_now[span] += sum_in[t - 1, span].astype(F32)

            @pl.when(t < RING - 1)
            def _(member=member, span=span):
                sum_out[t, span] = down_now[span].astype(BF)
                sum_on(member, t + 1).start()

    forward(0, 1).start()
    send_weights(len(pending))
    for copy in across:
        copy.wait_recv()
    for d in (1, 3, 2):
        spread[d - 1].wait_recv()
        forward(d, 1).start()
    copies += spread
    stages = (stage_a, stage_b, stage_c, stage_e)

    def turn(t, carry):
        for lag in (0, 3, 2, 1):
            @pl.when(jnp.logical_and(t >= lag, t < RING + lag))
            def _(lag=lag):
                stages[lag](t - lag)

        return carry

    lax.fori_loop(0, RING + 3, turn, 0)
    back = {}
    for member in (2, 3, 1, 0):
        span = pl.ds(member * CAP, CAP)
        sum_on(member, RING - 1).wait_recv()
        down_own[span] += sum_in[RING - 2, span].astype(F32)
        if member:
            back_out[span] = down_own[span].astype(BF)
            back[member] = remote(
                back_out.at[span], back_in.at[member], back_send.at[member], back_recv.at[member],
                first_axis(y, z, core, RING - member * stride),
            )
            back[member].start()
    mlp = down_own[0:CAP, :]
    for d in range(1, MEMBERS):
        back[d].wait_recv()
        mlp = mlp + back_in[d].astype(F32)
    mlp = mlp.astype(BF).astype(F32)
    result = x_rows + router * (attn[...] + mlp)
    out_ref[...] = jnp.where(live, result, 0.0).astype(BF)
    for copy in copies + list(back.values()):
        copy.wait_send()
    for kind in range(2):
        for dest in (2, 3):
            all_of(kind, dest).wait_send()

    def drain(t, carry):
        for copy in [x_one(t), x_two(t)] + [x_hidden(d, t) for d in range(1, TP)]:
            copy.wait_send()

        @pl.when(t >= 1)
        def _():
            for member in range(MEMBERS):
                forward(member, t).wait_send()
                sum_on(member, t).wait_send()

        return carry

    lax.fori_loop(0, RING, drain, 0)


def vmem(count):
    return [pl.BlockSpec(memory_space=pltpu.VMEM)] * count


SCALAR = pl.BlockSpec(memory_space=pltpu.SMEM)
DMA = pltpu.SemaphoreType.DMA


def local(
    resid, query, key, value, router_logit, norm_gain, w_gate, w_up, w_down, sel_index, sel_count
):
    width = resid.shape[1]
    tall = width // key.shape[1] * CAP
    heads = key.shape[1] // HEAD_DIM
    units = w_down.shape[0]
    whole = MEMBERS * CAP
    hid = BLOCKS * units
    return pl.pallas_call(
        block_kernel,
        out_shape=jax.ShapeDtypeStruct((CAP, width), BF),
        in_specs=[pl.BlockSpec(memory_space=pl.ANY)] * 10 + [SCALAR],
        out_specs=vmem(1)[0],
        scratch_shapes=[
            pltpu.VMEM(resid.shape, BF),
            pltpu.VMEM(query.shape, BF),
            pltpu.VMEM(key.shape, BF),
            pltpu.VMEM(value.shape, BF),
            pltpu.VMEM((1, router_logit.shape[0]), F32),
            pltpu.VMEM((1, norm_gain.shape[0]), BF),
            pltpu.VMEM(sel_index.shape, jnp.int32),
            DMA((10,)),
            pltpu.VMEM((2, RING, RING, CAP, 2 * key.shape[1]), BF),
            pltpu.VMEM((heads, tall + 16, HEAD_DIM), BF),
            pltpu.VMEM((heads, tall, 1), F32),
            pltpu.VMEM((heads, tall, 1), F32),
            pltpu.VMEM((heads, tall, HEAD_DIM), F32),
            pltpu.VMEM((TP, CAP, HEAD_DIM), F32),
            pltpu.VMEM((1, RING * CAP), F32),
            pltpu.VMEM((CAP, width), F32),
            pltpu.VMEM((2, BLOCKS, units, width), BF),
            pltpu.VMEM((BLOCKS, units, width), BF),
            pltpu.VMEM((RING, whole, width), BF),
            pltpu.VMEM((2, whole, 2 * hid), F32),
            pltpu.VMEM((2, whole // 4, 2 * hid), F32),
            pltpu.VMEM((RING, whole // 2, 2 * hid), BF),
            pltpu.VMEM((RING, whole // 2, 2 * hid), BF),
            pltpu.VMEM((RING, whole // 4, 2 * hid), BF),
            pltpu.VMEM((RING, whole // 4, 2 * hid), BF),
            pltpu.VMEM((RING, whole, hid), BF),
            pltpu.VMEM((RING - 1, whole, width), BF),
            pltpu.VMEM((RING - 1, whole, width), BF),
            pltpu.VMEM((whole, width), F32),
            pltpu.VMEM((whole, width), F32),
            pltpu.VMEM((whole, width), BF),
            pltpu.VMEM((MEMBERS, CAP, width), BF),
            DMA((RING,)), DMA((RING,)),
            DMA((2, RING // 2 + 1, RING)), DMA((2, RING // 2 + 1, RING)),
            DMA((RING, SHARES)), DMA((RING, SHARES)),
            DMA((TP,)), DMA((TP,)),
            DMA((2, 3)), DMA((2, 3)),
            DMA((MEMBERS,)), DMA((MEMBERS,)),
            DMA((MEMBERS, RING)), DMA((MEMBERS, RING)),
            DMA((2, RING)), DMA((2, RING)),
            DMA((TP, RING)), DMA((TP, RING)),
            DMA((MEMBERS, RING)), DMA((MEMBERS, RING)),
            DMA((MEMBERS,)), DMA((MEMBERS,)),
        ],
        compiler_params=pltpu.CompilerParams(collective_id=0, has_side_effects=True),
        name="block",
    )(
        resid, query, key, value, router_logit[None, :], norm_gain[None, :], sel_index,
        w_gate.T, w_up.T, w_down, sel_count,
    )


def solution(mesh):
    split = Mesh(mesh.devices.reshape(8, 8, 2, mesh.shape["tp"]), (*CTX, "tp"))
    placed = (
        P(CTX, "tp"),
        P(CTX, "tp"),
        P(CTX, "tp"),
        P(CTX, "tp"),
        P(CTX),
        P("tp"),
        P("tp", CTX),
        P("tp", CTX),
        P(CTX, "tp"),
        P(CTX, None),
        P(CTX),
    )
    return jax.shard_map(
        local, mesh=split, in_specs=placed, out_specs=P(CTX, "tp"), check_vma=False
    )
```

```python
import functools

import jax
import jax.numpy as jnp
from jax import lax
from jax.experimental import pallas as pl
from jax.experimental.pallas import tpu as pltpu
from jax.sharding import Mesh
from jax.sharding import PartitionSpec as P

D = 4096
HEAD_DIM = 128
CAP = 32
RING = 8
TP = 4
NEG = -1e30
EPSILON = 1e-05
DEAD = 64.0
KEY_LIMIT = 8.0
CTX = ("cy", "cz", "cc")
MESH = pl.DeviceIdType.MESH
BF = jnp.bfloat16
F32 = jnp.float32
SHARES = 2
ORDER = (0, 1, 7, 2, 6, 3, 5, 4)
MEMBERS = 4
PACE = 3
LAGS = (0, 1, 2, 3)
BLOCKS = 4


def dot(a, b):
    return jnp.dot(a, b, preferred_element_type=F32)


def dot_t(a, b):
    return lax.dot_general(a, b, (((1,), (1,)), ((), ())), preferred_element_type=F32)


def place():
    y, z = lax.axis_index("cy"), lax.axis_index("cz")
    core, x = lax.axis_index("cc"), lax.axis_index("tp")
    return y, z, core, x


def wrap(value):
    return lax.rem(value + RING, RING)


def kin(y, z, core, step, turned):
    at_core = core if step % 2 == 0 else 1 - core
    return {
        "cy": wrap(y + step * (1 - turned)), "cz": wrap(z + step * turned), "cc": at_core,
    }


def first_axis(y, z, core, step):
    return kin(y, z, core, step, lane_of(y, z, core))


def second_axis(y, z, core, step):
    return kin(y, z, core, step, 1 - lane_of(y, z, core))


def lane_of(y, z, core):
    return lax.rem(core + y + z, 2)


def beside(y, z, core, turned):
    step = 1 - 2 * lax.rem(y * (1 - turned) + z * turned, 2)
    return {"cy": y + step * (1 - turned), "cz": z + step * turned}


def other_core(core):
    return {"cc": 1 - core}


def remote(src, dst, send, recv, device):
    return pltpu.make_async_remote_copy(
        src_ref=src, dst_ref=dst, send_sem=send, recv_sem=recv, device_id=device, device_id_type=MESH
    )


def greet(devices):
    barrier = pltpu.get_barrier_semaphore()
    for device in devices:
        pl.semaphore_signal(barrier, inc=1, device_id=device, device_id_type=MESH)
    return lambda: pl.semaphore_wait(barrier, len(devices))


def block_kernel(
    resid_hbm, query_hbm, key_hbm, value_hbm, logit_hbm, gain_hbm, picked_hbm, w_gate, w_up, w_down,
    count,
    out_ref,
    resid, query, key, value, logit, gain, picked_at, load_sem,
    kv, q_ext, top, total, accum, squares, idx_wide, attn,
    gate_up, down_w, rows, part_sum, quarter, half_out, half_in, quarter_out, quarter_in,
    hidden, sum_out, sum_in, down_now, down_own, back_out, back_in,
    near_send, near_recv, far_send, far_recv, chip_send, chip_recv, sq_send, sq_recv,
    w_send, w_recv, row_send, row_recv, ring_send, ring_recv, x_send, x_recv, y_send, y_recv,
    sum_send, sum_recv, back_send, back_recv,
):
    y, z, core, x = place()
    shard = y * 16 + z * 2 + core
    side = lane_of(y, z, core)
    twin = {**beside(y, z, core, side), "cc": 1 - core}
    cross = {**beside(y, z, core, 1 - side), "cc": core}
    cross_from = {**beside(y, z, core, side), "cc": core}
    up = second_axis(y, z, core, 1)
    down = second_axis(y, z, core, RING - 1)
    units = w_gate.shape[0]
    loads = []
    for n, (src, dst) in enumerate(
        (
            (picked_hbm, picked_at), (key_hbm, key), (value_hbm, value), (resid_hbm, resid),
            (query_hbm, query), (logit_hbm, logit), (gain_hbm, gain), (w_gate, gate_up.at[0, 0]),
            (w_up, gate_up.at[1, 0]), (w_down, down_w.at[0]),
        )
    ):
        loads.append(pltpu.make_async_copy(src, dst, load_sem.at[n]))
        loads[-1].start()
    entered = greet(
        [first_axis(y, z, core, d) for d in range(1, RING)]
        + [up, down, other_core(core), cross, cross_from]
        + [{"tp": lax.rem(x + d, TP)} for d in range(1, TP)]
    )
    for load in loads[0:3]:
        load.wait()
    width = resid.shape[1]
    kv_width = key.shape[1]
    heads = kv_width // HEAD_DIM
    group = width // kv_width
    row_f = picked_at[...].astype(F32)
    eye = lax.broadcasted_iota(jnp.int32, (CAP, CAP), 0) == lax.broadcasted_iota(
        jnp.int32, (CAP, CAP), 1
    )
    col_f = jnp.sum(jnp.where(eye, row_f, 0.0), axis=1, keepdims=True)
    spots = lax.broadcasted_iota(jnp.int32, (CAP, resid.shape[0]), 1).astype(F32)
    picks = col_f == spots
    onehot = jnp.where(picks, 1.0, 0.0).astype(BF)
    live = lax.broadcasted_iota(jnp.int32, (CAP, 1), 0) < count[0]
    keys = jnp.where(live, dot(onehot, key[...]), DEAD)
    kv[0, 0, 0, :, 0:kv_width] = keys.astype(BF)
    kv[0, 0, 0, :, kv_width : 2 * kv_width] = dot(onehot, value[...]).astype(BF)
    entered()
    copies = []
    near = {}
    for d in (4, 3, 5, 2, 6, 1, 7):
        near[d] = remote(
            kv.at[0, 0, 0], kv.at[0, 0, d], near_send.at[0], near_recv.at[d],
            first_axis(y, z, core, d),
        )
        near[d].start()
    steps = (RING // 2, RING // 2 - 1)
    started = {}

    def launch(way, step, wave):
        src = step - 1 if way == 0 else (RING - step + 1) % RING
        dst = step if way == 0 else RING - step
        started[way, step, wave] = remote(
            kv.at[0, src, wave], kv.at[0, dst, wave],
            far_send.at[0], far_recv.at[way * 4 + step - 1, wave], up if way == 0 else down,
        )
        started[way, step, wave].start()

    shared = {}
    part = RING // SHARES

    def share(slot, piece):
        span = pl.ds(piece * part, part)
        shared[slot, piece] = remote(
            kv.at[0, slot, span], kv.at[1, slot, span],
            chip_send.at[0], chip_recv.at[slot, piece], other_core(core),
        )
        shared[slot, piece].start()

    for way in range(2):
        launch(way, 1, 0)
    for load in loads[3:]:
        load.wait()
    across = [
        remote(
            gate_up.at[:, 0], gate_up.at[:, 1], w_send.at[0, 0], w_recv.at[0, 0], other_core(core)
        ),
        remote(down_w.at[0], down_w.at[1], w_send.at[1, 0], w_recv.at[1, 0], other_core(core)),
    ]
    for copy in across:
        copy.start()
    weight_span = 16
    pending = []
    for kind in range(2):
        for at in range(0, units, weight_span):
            for dest, device in ((2, twin), (3, cross)):
                pending.append((kind, at, dest, device))

    def send_weights(number):
        for kind, at, dest, device in pending[:number]:
            span = pl.ds(at, weight_span)
            if kind == 0:
                src, dst = gate_up.at[:, 0, span], gate_up.at[:, dest, span]
            else:
                src, dst = down_w.at[0, span], down_w.at[dest, span]
            remote(src, dst, w_send.at[kind, dest - 1], w_recv.at[kind, dest - 1], device).start()
        del pending[:number]

    def all_of(kind, dest):
        if kind == 0:
            src, dst = gate_up.at[:, 0], gate_up.at[:, dest]
        else:
            src, dst = down_w.at[0], down_w.at[dest]
        return remote(src, dst, w_send.at[kind, dest - 1], w_recv.at[kind, dest - 1], twin)

    x_rows = dot(onehot, resid[...])
    q_rows = dot(onehot, query[...]).astype(BF)
    q_tall = group * CAP
    unit = jnp.where(lax.broadcasted_iota(jnp.int32, (16, HEAD_DIM), 1) == 0, 1.0, 0.0).astype(BF)
    for h in range(heads):
        for g in range(group):
            at = (h * group + g) * HEAD_DIM
            q_ext[h, g * CAP : (g + 1) * CAP, :] = q_rows[:, at : at + HEAD_DIM]
        q_ext[h, q_tall : q_tall + 16, :] = unit
    chosen = jnp.sum(jnp.where(picks, logit[...], 0.0), axis=1, keepdims=True)
    router = 1.0 / (1.0 + jnp.exp(-chosen))
    idx_wide[...] = jnp.zeros(idx_wide.shape, F32)
    idx_wide[:, 0:CAP] = row_f
    idx_tall = jnp.concatenate([col_f] * group, axis=0)
    top[...] = jnp.full(top.shape, NEG, F32)
    total[...] = jnp.zeros(total.shape, F32)
    accum[...] = jnp.zeros(accum.shape, F32)
    scale = HEAD_DIM ** (-0.5)
    block = RING * CAP
    lane = lax.broadcasted_iota(jnp.int32, (1, block), 1)

    def attend(slot, cls, own):
        kind = side + cls - 2 * side * cls
        mine1 = y * (1 - kind) + z * kind
        mine2 = z * (1 - kind) + y * kind
        from1 = jnp.bitwise_and(mine1 + RING - lax.shift_right_logical(lane, 5), RING - 1)
        from2 = wrap(mine2 - slot)
        at_core = jnp.bitwise_and(from1 + from2 + kind, 1)
        source = (
            16 * (from1 * (1 - kind) + from2 * kind) + 2 * (from2 * (1 - kind) + from1 * kind) + at_core
        )
        piece = kv[cls, slot].reshape(block, 2 * kv_width)
        for h in range(heads):
            k_part = piece[:, h * HEAD_DIM : (h + 1) * HEAD_DIM]
            v_part = piece[:, kv_width + h * HEAD_DIM : kv_width + (h + 1) * HEAD_DIM]
            both = dot_t(q_ext[h], k_part)
            alive = both[q_tall : q_tall + 1, :] <= KEY_LIMIT
            allowed = source < shard
            if own:
                same = jnp.logical_and(source == shard, idx_wide[...] <= idx_tall)
                allowed = jnp.logical_or(allowed, same)
            allowed = jnp.logical_and(allowed, alive)
            scores = jnp.where(allowed, both[0:q_tall, :] * scale, NEG)
            before = top[h]
            now = jnp.maximum(before, jnp.max(scores, axis=1, keepdims=True))
            prob = jnp.exp(scores - now)
            fade = jnp.exp(before - now)
            top[h] = now
            total[h] = total[h] * fade + jnp.sum(prob, axis=1, keepdims=True)
            accum[h] = accum[h] * fade + dot(prob.astype(BF), v_part)

    for wave in ORDER:
        if wave:
            near[wave].wait_recv()
            for way in range(2):
                launch(way, 1, wave)
        if wave == 3:
            share(0, 0)
    share(0, 1)
    todo = [(0, 0), (0, 1)]

    def attend_next():
        slot, cls = todo.pop(0)
        if cls:
            for piece in range(SHARES):
                shared[slot, piece].wait_recv()
        attend(slot, cls, (slot, cls) == (0, 0))

    for step in range(1, RING // 2 + 1):
        for n, wave in enumerate(ORDER):
            for way in range(2):
                if step <= steps[way]:
                    started[way, step, wave].wait_recv()
                    if step < steps[way]:
                        launch(way, step + 1, wave)
                    if wave in (3, 4):
                        share(step if way == 0 else RING - step, wave - 3)
            if n % 2 and todo:
                attend_next()
        todo += [(step, 0), (RING - step, 0), (step, 1), (RING - step, 1)] if step < 4 else []
        send_weights(PACE)
    attend(RING // 2, 0, False)
    for piece in range(SHARES):
        shared[RING // 2, piece].wait_recv()
    attend(RING // 2, 1, False)
    copies += across
    for h in range(heads):
        mixed = accum[h] / total[h]
        for g in range(group):
            at = (h * group + g) * HEAD_DIM
            attn[:, at : at + HEAD_DIM] = mixed[g * CAP : (g + 1) * CAP, :]
    h_one = (x_rows + attn[...]).astype(BF).astype(F32)
    squares[0] = jnp.broadcast_to(jnp.sum(h_one * h_one, axis=1, keepdims=True), squares.shape[1:])
    sums = []
    for d in range(1, TP):
        sums.append(
            remote(squares.at[0], squares.at[d], sq_send.at[0], sq_recv.at[0], {"tp": lax.rem(x + d, TP)})
        )
        sums[-1].start()
    send_weights(8)
    theirs = squares.at[pl.ds(1, TP - 1)]
    remote(theirs, theirs, sq_send.at[0], sq_recv.at[0], twin).wait_recv()
    whole_sum = squares[0] + squares[1] + squares[2] + squares[3]
    rscale = lax.rsqrt(whole_sum[:, 0:1] / D + EPSILON)
    rows[0, 0:CAP, :] = (h_one * gain[...].astype(F32) * rscale).astype(BF)

    stride = RING // MEMBERS
    whole = MEMBERS * CAP
    half = whole // 2
    fourth = whole // 4
    hid = BLOCKS * units
    low, high = lax.rem(x, 2), lax.div(x, 2)
    odd = lax.rem(low + high, 2)
    flip = x + 1 - 2 * low
    mirror = TP - 1 - x
    first_x = {"tp": flip * (1 - core) + mirror * core}
    second_x = {"tp": mirror * (1 - core) + flip * core}
    keep_half = odd * (1 - core) + high * core
    keep_fourth = high * (1 - core) + low * core
    spread = []
    for d in range(1, MEMBERS):
        spread.append(
            remote(
                rows.at[0, pl.ds(0, CAP)], rows.at[0, pl.ds(d * CAP, CAP)],
                row_send.at[0], row_recv.at[d], first_axis(y, z, core, d * stride),
            )
        )
    for d in (2, 1, 3):
        spread[d - 1].start()

    def forward(member, step):
        span = pl.ds(member * CAP, CAP)
        return remote(
            rows.at[step - 1, span], rows.at[step, span], ring_send.at[0],
            ring_recv.at[member, step], up if member < MEMBERS // 2 else down,
        )

    def sum_on(member, step):
        span = pl.ds(member * CAP, CAP)
        return remote(
            sum_out.at[step - 1, span], sum_in.at[step - 1, span], sum_send.at[0],
            sum_recv.at[member, step], up if member < MEMBERS // 2 else down,
        )

    my_half = pl.multiple_of(keep_half * half, half)
    its_half = pl.multiple_of((1 - keep_half) * half, half)
    my_fourth = pl.multiple_of(keep_fourth * fourth, fourth)
    its_fourth = pl.multiple_of((1 - keep_fourth) * fourth, fourth)
    mine = pl.multiple_of(my_half + my_fourth, fourth)

    def x_one(t):
        return remote(half_out.at[t], half_in.at[t], x_send.at[0], x_recv.at[0, t], first_x)

    def x_two(t):
        return remote(quarter_out.at[t], quarter_in.at[t], x_send.at[1], x_recv.at[1, t], second_x)

    def x_hidden(d, t):
        span = pl.ds(mine, fourth)
        return remote(
            hidden.at[t, span], hidden.at[t, span], y_send.at[0], y_recv.at[t],
            {"tp": lax.rem(x + d, TP)},
        )

    def stage_a(t):
        for member in (0, 2, 1, 3):
            @pl.when(t < RING - 1)
            def _(member=member):
                forward(member, t + 1).wait_recv()

            @pl.when(t < RING - 2)
            def _(member=member):
                forward(member, t + 2).start()

        @pl.when(t == 0)
        def _():
            for dest in (2, 3):
                all_of(0, dest).wait_recv()

        slot = lax.rem(t, 2)
        part_sum[slot] = dot_t(rows[lax.rem(t + 1, RING)], gate_up[...].reshape(2 * hid, width))
        half_out[t] = part_sum[slot, pl.ds(its_half, half)].astype(BF)
        x_one(t).start()

    def stage_b(t):
        slot = lax.rem(t, 2)
        x_one(t).wait_recv()
        sent = part_sum[slot, pl.ds(pl.multiple_of(my_half + its_fourth, fourth), fourth)]
        quarter_out[t] = (sent + half_in[t, pl.ds(its_fourth, fourth)].astype(F32)).astype(BF)
        x_two(t).start()
        kept = part_sum[slot, pl.ds(mine, fourth)]
        quarter[slot] = kept + half_in[t, pl.ds(my_fourth, fourth)].astype(F32)

    def stage_c(t):
        slot = lax.rem(t, 2)
        x_two(t).wait_recv()
        both = quarter[slot] + quarter_in[t].astype(F32)
        gate, up_val = both[:, 0:hid], both[:, hid : 2 * hid]
        hidden[t, pl.ds(mine, fourth)] = (gate / (1.0 + jnp.exp(-gate)) * up_val).astype(BF)
        for d in (2, 1, 3):
            x_hidden(d, t).start()

    def stage_e(t):
        @pl.when(t == 0)
        def _():
            for dest in (2, 3):
                all_of(1, dest).wait_recv()

        span = pl.ds(0, whole - fourth)
        remote(
            hidden.at[t, span], hidden.at[t, span], y_send.at[0], y_recv.at[t], twin
        ).wait_recv()
        down_now[...] = dot(hidden[t], down_w[...].reshape(hid, width))

        @pl.when(t == RING - 1)
        def _():
            down_own[...] = down_now[...]

        for member in (0, 2, 1, 3):
            span = pl.ds(member * CAP, CAP)

            @pl.when(jnp.logical_and(t >= 1, t < RING - 1))
            def _(member=member, span=span):
                sum_on(member, t).wait_recv()
                down_now[span] += sum_in[t - 1, span].astype(F32)

            @pl.when(t < RING - 1)
            def _(member=member, span=span):
                sum_out[t, span] = down_now[span].astype(BF)
                sum_on(member, t + 1).start()

    forward(0, 1).start()
    send_weights(len(pending))
    for copy in across:
        copy.wait_recv()
    for d in (1, 3, 2):
        spread[d - 1].wait_recv()
        forward(d, 1).start()
    stages = (stage_a, stage_b, stage_c, stage_e)

    def turn(t, carry):
        for lag in LAGS:
            @pl.when(jnp.logical_and(t >= lag, t < RING + lag))
            def _(lag=lag):
                stages[lag](t - lag)

        return carry

    lax.fori_loop(0, RING + 3, turn, 0)
    back = {}
    for member in (2, 3, 1, 0):
        span = pl.ds(member * CAP, CAP)
        sum_on(member, RING - 1).wait_recv()
        down_own[span] += sum_in[RING - 2, span].astype(F32)
        if member:
            back_out[span] = down_own[span].astype(BF)
            back[member] = remote(
                back_out.at[span], back_in.at[member], back_send.at[0], back_recv.at[member],
                first_axis(y, z, core, RING - member * stride),
            )
            back[member].start()
    mlp = down_own[0:CAP, :]
    for d in range(1, MEMBERS):
        back[d].wait_recv()
        mlp = mlp + back_in[d].astype(F32)
    mlp = mlp.astype(BF).astype(F32)
    result = x_rows + router * (attn[...] + mlp)
    out_ref[...] = jnp.where(live, result, 0.0).astype(BF)
    for copy in copies:
        copy.wait_send()
    for kind in range(2):
        for dest in (2, 3):
            all_of(kind, dest).wait_send()
    others = pl.ds(CAP, whole - CAP)
    for ref, sem in (
        (kv.at[0, 0, pl.ds(1, RING - 1)], near_send.at[0]),
        (kv.at[0, pl.ds(1, RING - 1)], far_send.at[0]),
        (kv.at[1], chip_send.at[0]),
        (squares.at[pl.ds(1, TP - 1)], sq_send.at[0]),
        (rows.at[0, others], row_send.at[0]),
        (rows.at[pl.ds(1, RING - 1)], ring_send.at[0]),
        (sum_out, sum_send.at[0]),
        (half_out, x_send.at[0]),
        (quarter_out, x_send.at[1]),
        (hidden.at[:, pl.ds(0, whole - fourth)], y_send.at[0]),
        (back_out.at[others], back_send.at[0]),
    ):
        remote(ref, ref, sem, sem, twin).wait_send()


def vmem(count):
    return [pl.BlockSpec(memory_space=pltpu.VMEM)] * count


SCALAR = pl.BlockSpec(memory_space=pltpu.SMEM)
DMA = pltpu.SemaphoreType.DMA


def local(
    resid, query, key, value, router_logit, norm_gain, w_gate, w_up, w_down, sel_index, sel_count
):
    width = resid.shape[1]
    tall = width // key.shape[1] * CAP
    heads = key.shape[1] // HEAD_DIM
    units = w_down.shape[0]
    whole = MEMBERS * CAP
    hid = BLOCKS * units
    return pl.pallas_call(
        block_kernel,
        out_shape=jax.ShapeDtypeStruct((CAP, width), BF),
        in_specs=[pl.BlockSpec(memory_space=pl.ANY)] * 10 + [SCALAR],
        out_specs=vmem(1)[0],
        scratch_shapes=[
            pltpu.VMEM(resid.shape, BF),
            pltpu.VMEM(query.shape, BF),
            pltpu.VMEM(key.shape, BF),
            pltpu.VMEM(value.shape, BF),
            pltpu.VMEM((1, router_logit.shape[0]), F32),
            pltpu.VMEM((1, norm_gain.shape[0]), BF),
            pltpu.VMEM(sel_index.shape, jnp.int32),
            DMA((10,)),
            pltpu.VMEM((2, RING, RING, CAP, 2 * key.shape[1]), BF),
            pltpu.VMEM((heads, tall + 16, HEAD_DIM), BF),
            pltpu.VMEM((heads, tall, 1), F32),
            pltpu.VMEM((heads, tall, 1), F32),
            pltpu.VMEM((heads, tall, HEAD_DIM), F32),
            pltpu.VMEM((TP, CAP, HEAD_DIM), F32),
            pltpu.VMEM((1, RING * CAP), F32),
            pltpu.VMEM((CAP, width), F32),
            pltpu.VMEM((2, BLOCKS, units, width), BF),
            pltpu.VMEM((BLOCKS, units, width), BF),
            pltpu.VMEM((RING, whole, width), BF),
            pltpu.VMEM((2, whole, 2 * hid), F32),
            pltpu.VMEM((2, whole // 4, 2 * hid), F32),
            pltpu.VMEM((RING, whole // 2, 2 * hid), BF),
            pltpu.VMEM((RING, whole // 2, 2 * hid), BF),
            pltpu.VMEM((RING, whole // 4, 2 * hid), BF),
            pltpu.VMEM((RING, whole // 4, 2 * hid), BF),
            pltpu.VMEM((RING, whole, hid), BF),
            pltpu.VMEM((RING - 1, whole, width), BF),
            pltpu.VMEM((RING - 1, whole, width), BF),
            pltpu.VMEM((whole, width), F32),
            pltpu.VMEM((whole, width), F32),
            pltpu.VMEM((whole, width), BF),
            pltpu.VMEM((MEMBERS, CAP, width), BF),
            DMA((1,)), DMA((RING,)),
            DMA((1,)), DMA((RING - 1, RING)),
            DMA((1,)), DMA((RING, SHARES)),
            DMA((1,)), DMA((1,)),
            DMA((2, 3)), DMA((2, 3)),
            DMA((1,)), DMA((MEMBERS,)),
            DMA((1,)), DMA((MEMBERS, RING)),
            DMA((2,)), DMA((2, RING)),
            DMA((1,)), DMA((RING,)),
            DMA((1,)), DMA((MEMBERS, RING)),
            DMA((1,)), DMA((MEMBERS,)),
        ],
        compiler_params=pltpu.CompilerParams(collective_id=0, has_side_effects=True),
        name="block",
    )(
        resid, query, key, value, router_logit[None, :], norm_gain[None, :], sel_index,
        w_gate.T, w_up.T, w_down, sel_count,
    )


def solution(mesh):
    split = Mesh(mesh.devices.reshape(8, 8, 2, mesh.shape["tp"]), (*CTX, "tp"))
    placed = (
        P(CTX, "tp"),
        P(CTX, "tp"),
        P(CTX, "tp"),
        P(CTX, "tp"),
        P(CTX),
        P("tp"),
        P("tp", CTX),
        P("tp", CTX),
        P(CTX, "tp"),
        P(CTX, None),
        P(CTX),
    )
    return jax.shard_map(
        local, mesh=split, in_specs=placed, out_specs=P(CTX, "tp"), check_vma=False
    )
```

```python
import functools

import jax
import jax.numpy as jnp
from jax import lax
from jax.experimental import pallas as pl
from jax.experimental.pallas import tpu as pltpu
from jax.sharding import Mesh
from jax.sharding import PartitionSpec as P

D = 4096
HEAD_DIM = 128
CAP = 32
RING = 8
TP = 4
NEG = -1e30
EPSILON = 1e-05
DEAD = 64.0
KEY_LIMIT = 8.0
CTX = ("cy", "cz", "cc")
MESH = pl.DeviceIdType.MESH
BF = jnp.bfloat16
F32 = jnp.float32
SHARES = 2
ORDER = (0, 1, 7, 2, 6, 3, 5, 4)
MEMBERS = 4
PACE = 2
LAGS = (0, 1, 2, 3)
BLOCKS = 4


def dot(a, b):
    return jnp.dot(a, b, preferred_element_type=F32)


def dot_t(a, b):
    return lax.dot_general(a, b, (((1,), (1,)), ((), ())), preferred_element_type=F32)


def place():
    y, z = lax.axis_index("cy"), lax.axis_index("cz")
    core, x = lax.axis_index("cc"), lax.axis_index("tp")
    return y, z, core, x


def wrap(value):
    return lax.rem(value + RING, RING)


def kin(y, z, core, step, turned):
    at_core = core if step % 2 == 0 else 1 - core
    return {
        "cy": wrap(y + step * (1 - turned)), "cz": wrap(z + step * turned), "cc": at_core,
    }


def first_axis(y, z, core, step):
    return kin(y, z, core, step, lane_of(y, z, core))


def second_axis(y, z, core, step):
    return kin(y, z, core, step, 1 - lane_of(y, z, core))


def lane_of(y, z, core):
    return lax.rem(core + y + z, 2)


def beside(y, z, core, turned):
    step = 1 - 2 * lax.rem(y * (1 - turned) + z * turned, 2)
    return {"cy": y + step * (1 - turned), "cz": z + step * turned}


def other_core(core):
    return {"cc": 1 - core}


def remote(src, dst, send, recv, device):
    return pltpu.make_async_remote_copy(
        src_ref=src, dst_ref=dst, send_sem=send, recv_sem=recv, device_id=device, device_id_type=MESH
    )


def greet(devices):
    barrier = pltpu.get_barrier_semaphore()
    for device in devices:
        pl.semaphore_signal(barrier, inc=1, device_id=device, device_id_type=MESH)
    return lambda: pl.semaphore_wait(barrier, len(devices))


def block_kernel(
    resid_hbm, query_hbm, key_hbm, value_hbm, logit_hbm, gain_hbm, picked_hbm, w_gate, w_up, w_down,
    count,
    out_ref,
    resid, query, key, value, logit, gain, picked_at, load_sem,
    kv, q_ext, top, total, accum, squares, idx_wide, attn,
    gate_up, down_w, rows, raw, tiles, part_sum, quarter, half_out, half_in, quarter_out, quarter_in,
    hidden, sum_out, sum_in, down_now, down_own, back_out, back_in,
    near_send, near_recv, far_send, far_recv, chip_send, chip_recv, sq_send, sq_recv,
    w_send, w_recv, row_send, row_recv, tile_send, tile_recv, ring_send, ring_recv, x_send, x_recv, y_send, y_recv,
    sum_send, sum_recv, back_send, back_recv,
):
    y, z, core, x = place()
    shard = y * 16 + z * 2 + core
    side = lane_of(y, z, core)
    twin = {**beside(y, z, core, side), "cc": 1 - core}
    cross = {**beside(y, z, core, 1 - side), "cc": core}
    cross_from = {**beside(y, z, core, side), "cc": core}
    up = second_axis(y, z, core, 1)
    down = second_axis(y, z, core, RING - 1)
    units = w_gate.shape[0]
    loads = []
    for n, (src, dst) in enumerate(
        (
            (picked_hbm, picked_at), (key_hbm, key), (value_hbm, value), (resid_hbm, resid),
            (query_hbm, query), (logit_hbm, logit), (gain_hbm, gain), (w_gate, gate_up.at[0, 0]),
            (w_up, gate_up.at[1, 0]), (w_down, down_w.at[0]),
        )
    ):
        loads.append(pltpu.make_async_copy(src, dst, load_sem.at[n]))
        loads[-1].start()
    entered = greet(
        [first_axis(y, z, core, d) for d in range(1, RING)]
        + [up, down, other_core(core), cross, cross_from]
        + [{"tp": lax.rem(x + d, TP)} for d in range(1, TP)]
    )
    for load in loads[0:3]:
        load.wait()
    width = resid.shape[1]
    kv_width = key.shape[1]
    heads = kv_width // HEAD_DIM
    group = width // kv_width
    row_f = picked_at[...].astype(F32)
    eye = lax.broadcasted_iota(jnp.int32, (CAP, CAP), 0) == lax.broadcasted_iota(
        jnp.int32, (CAP, CAP), 1
    )
    col_f = jnp.sum(jnp.where(eye, row_f, 0.0), axis=1, keepdims=True)
    spots = lax.broadcasted_iota(jnp.int32, (CAP, resid.shape[0]), 1).astype(F32)
    picks = col_f == spots
    onehot = jnp.where(picks, 1.0, 0.0).astype(BF)
    live = lax.broadcasted_iota(jnp.int32, (CAP, 1), 0) < count[0]
    keys = jnp.where(live, dot(onehot, key[...]), DEAD)
    kv[0, 0, 0, :, 0:kv_width] = keys.astype(BF)
    kv[0, 0, 0, :, kv_width : 2 * kv_width] = dot(onehot, value[...]).astype(BF)
    entered()
    copies = []
    near = {}
    for d in (4, 3, 5, 2, 6, 1, 7):
        near[d] = remote(
            kv.at[0, 0, 0], kv.at[0, 0, d], near_send.at[0], near_recv.at[d],
            first_axis(y, z, core, d),
        )
        near[d].start()
    steps = (RING // 2, RING // 2 - 1)
    started = {}

    def launch(way, step, wave):
        src = step - 1 if way == 0 else (RING - step + 1) % RING
        dst = step if way == 0 else RING - step
        started[way, step, wave] = remote(
            kv.at[0, src, wave], kv.at[0, dst, wave],
            far_send.at[0], far_recv.at[way * 4 + step - 1, wave], up if way == 0 else down,
        )
        started[way, step, wave].start()

    part = RING // SHARES

    def share(slot, piece):
        span = pl.ds(piece * part, part)
        remote(
            kv.at[0, slot, span], kv.at[1, slot, span],
            chip_send.at[0], chip_recv.at[slot], other_core(core),
        ).start()

    def all_shared(slot):
        remote(
            kv.at[0, slot], kv.at[1, slot], chip_send.at[0], chip_recv.at[slot], other_core(core)
        ).wait_recv()

    for way in range(2):
        launch(way, 1, 0)
    for load in loads[3:]:
        load.wait()
    across = [
        remote(
            gate_up.at[:, 0], gate_up.at[:, 1], w_send.at[0, 0], w_recv.at[0, 0], other_core(core)
        ),
        remote(down_w.at[0], down_w.at[1], w_send.at[1, 0], w_recv.at[1, 0], other_core(core)),
    ]
    for copy in across:
        copy.start()
    weight_span = 16
    pending = []
    for kind in range(2):
        for at in range(0, units, weight_span):
            for dest, device in ((2, twin), (3, cross)):
                pending.append((kind, at, dest, device))

    def send_weights(number):
        for kind, at, dest, device in pending[:number]:
            span = pl.ds(at, weight_span)
            if kind == 0:
                src, dst = gate_up.at[:, 0, span], gate_up.at[:, dest, span]
            else:
                src, dst = down_w.at[0, span], down_w.at[dest, span]
            remote(src, dst, w_send.at[kind, dest - 1], w_recv.at[kind, dest - 1], device).start()
        del pending[:number]

    def all_of(kind, dest):
        if kind == 0:
            src, dst = gate_up.at[:, 0], gate_up.at[:, dest]
        else:
            src, dst = down_w.at[0], down_w.at[dest]
        return remote(src, dst, w_send.at[kind, dest - 1], w_recv.at[kind, dest - 1], twin)

    x_rows = dot(onehot, resid[...])
    q_rows = dot(onehot, query[...]).astype(BF)
    q_tall = group * CAP
    unit = jnp.where(lax.broadcasted_iota(jnp.int32, (16, HEAD_DIM), 1) == 0, 1.0, 0.0).astype(BF)
    for h in range(heads):
        for g in range(group):
            at = (h * group + g) * HEAD_DIM
            q_ext[h, g * CAP : (g + 1) * CAP, :] = q_rows[:, at : at + HEAD_DIM]
        q_ext[h, q_tall : q_tall + 16, :] = unit
    chosen = jnp.sum(jnp.where(picks, logit[...], 0.0), axis=1, keepdims=True)
    router = 1.0 / (1.0 + jnp.exp(-chosen))
    idx_wide[...] = jnp.zeros(idx_wide.shape, F32)
    idx_wide[:, 0:CAP] = row_f
    idx_tall = jnp.concatenate([col_f] * group, axis=0)
    top[...] = jnp.full(top.shape, NEG, F32)
    total[...] = jnp.zeros(total.shape, F32)
    accum[...] = jnp.zeros(accum.shape, F32)
    scale = HEAD_DIM ** (-0.5)
    block = RING * CAP
    lane = lax.broadcasted_iota(jnp.int32, (1, block), 1)

    def attend(slot, cls, own):
        kind = side + cls - 2 * side * cls
        mine1 = y * (1 - kind) + z * kind
        mine2 = z * (1 - kind) + y * kind
        from1 = jnp.bitwise_and(mine1 + RING - lax.shift_right_logical(lane, 5), RING - 1)
        from2 = wrap(mine2 - slot)
        at_core = jnp.bitwise_and(from1 + from2 + kind, 1)
        source = (
            16 * (from1 * (1 - kind) + from2 * kind) + 2 * (from2 * (1 - kind) + from1 * kind) + at_core
        )
        piece = kv[cls, slot].reshape(block, 2 * kv_width)
        for h in range(heads):
            k_part = piece[:, h * HEAD_DIM : (h + 1) * HEAD_DIM]
            v_part = piece[:, kv_width + h * HEAD_DIM : kv_width + (h + 1) * HEAD_DIM]
            both = dot_t(q_ext[h], k_part)
            alive = both[q_tall : q_tall + 1, :] <= KEY_LIMIT
            allowed = source < shard
            if own:
                same = jnp.logical_and(source == shard, idx_wide[...] <= idx_tall)
                allowed = jnp.logical_or(allowed, same)
            allowed = jnp.logical_and(allowed, alive)
            scores = jnp.where(allowed, both[0:q_tall, :] * scale, NEG)
            before = top[h]
            now = jnp.maximum(before, jnp.max(scores, axis=1, keepdims=True))
            prob = jnp.exp(scores - now)
            fade = jnp.exp(before - now)
            top[h] = now
            total[h] = total[h] * fade + jnp.sum(prob, axis=1, keepdims=True)
            accum[h] = accum[h] * fade + dot(prob.astype(BF), v_part)

    for wave in ORDER:
        if wave:
            near[wave].wait_recv()
            for way in range(2):
                launch(way, 1, wave)
        if wave == 3:
            share(0, 0)
    share(0, 1)
    todo = [(0, 0), (0, 1)]

    def attend_next():
        slot, cls = todo.pop(0)
        if cls:
            all_shared(slot)
        attend(slot, cls, (slot, cls) == (0, 0))

    for step in range(1, RING // 2 + 1):
        for n, wave in enumerate(ORDER):
            for way in range(2):
                if step <= steps[way]:
                    started[way, step, wave].wait_recv()
                    if step < steps[way]:
                        launch(way, step + 1, wave)
                    if wave in (3, 4):
                        share(step if way == 0 else RING - step, wave - 3)
            if n % 2 and todo:
                attend_next()
        todo += [(step, 0), (RING - step, 0), (step, 1), (RING - step, 1)] if step < 4 else []
        send_weights(PACE)
    attend(RING // 2, 0, False)
    all_shared(RING // 2)
    attend(RING // 2, 1, False)
    copies += across
    for h in range(heads):
        mixed = accum[h] / total[h]
        for g in range(group):
            at = (h * group + g) * HEAD_DIM
            attn[:, at : at + HEAD_DIM] = mixed[g * CAP : (g + 1) * CAP, :]
    h_one = (x_rows + attn[...]).astype(BF).astype(F32)
    squares[0] = jnp.broadcast_to(jnp.sum(h_one * h_one, axis=1, keepdims=True), squares.shape[1:])
    for d in range(1, TP):
        remote(
            squares.at[0], squares.at[d], sq_send.at[0], sq_recv.at[0], {"tp": lax.rem(x + d, TP)}
        ).start()
    raw[0] = (h_one * gain[...].astype(F32).reshape(1, width)).astype(BF)

    stride = RING // MEMBERS
    whole = MEMBERS * CAP
    half = whole // 2
    fourth = whole // 4
    hid = BLOCKS * units
    low, high = lax.rem(x, 2), lax.div(x, 2)
    odd = lax.rem(low + high, 2)
    flip = x + 1 - 2 * low
    mirror = TP - 1 - x
    first_x = {"tp": flip * (1 - core) + mirror * core}
    second_x = {"tp": mirror * (1 - core) + flip * core}
    keep_half = odd * (1 - core) + high * core
    keep_fourth = high * (1 - core) + low * core
    spread = {}
    scales = {}
    for d in (2, 1, 3):
        device = first_axis(y, z, core, d * stride)
        spread[d] = remote(raw.at[0], raw.at[d], row_send.at[0], row_recv.at[d], device)
        scales[d] = remote(tiles.at[0], tiles.at[d], tile_send.at[0], tile_recv.at[d], device)
        spread[d].start()
    send_weights(8)
    theirs = squares.at[pl.ds(1, TP - 1)]
    remote(theirs, theirs, sq_send.at[0], sq_recv.at[0], twin).wait_recv()
    whole_sum = squares[0] + squares[1] + squares[2] + squares[3]
    tiles[0] = lax.rsqrt(whole_sum / D + EPSILON)
    for d in (2, 1, 3):
        scales[d].start()

    def scale_rows(d):
        rows[0, d * CAP : (d + 1) * CAP, :] = (raw[d].astype(F32) * tiles[d, :, 0:1]).astype(BF)

    def forward(member, step):
        span = pl.ds(member * CAP, CAP)
        return remote(
            rows.at[step - 1, span], rows.at[step, span], ring_send.at[0],
            ring_recv.at[member, step], up if member < MEMBERS // 2 else down,
        )

    def sum_on(member, step):
        span = pl.ds(member * CAP, CAP)
        return remote(
            sum_out.at[step - 1, span], sum_in.at[step - 1, span], sum_send.at[0],
            sum_recv.at[member, step], up if member < MEMBERS // 2 else down,
        )

    my_half = pl.multiple_of(keep_half * half, half)
    its_half = pl.multiple_of((1 - keep_half) * half, half)
    my_fourth = pl.multiple_of(keep_fourth * fourth, fourth)
    its_fourth = pl.multiple_of((1 - keep_fourth) * fourth, fourth)
    mine = pl.multiple_of(my_half + my_fourth, fourth)

    def x_one(t):
        return remote(half_out.at[t], half_in.at[t], x_send.at[0], x_recv.at[0, t], first_x)

    def x_two(t):
        return remote(quarter_out.at[t], quarter_in.at[t], x_send.at[1], x_recv.at[1, t], second_x)

    def x_hidden(d, t):
        span = pl.ds(mine, fourth)
        return remote(
            hidden.at[t, span], hidden.at[t, span], y_send.at[0], y_recv.at[t],
            {"tp": lax.rem(x + d, TP)},
        )

    def stage_a(t):
        for member in (0, 2, 1, 3):
            @pl.when(t < RING - 1)
            def _(member=member):
                forward(member, t + 1).wait_recv()

            @pl.when(t < RING - 2)
            def _(member=member):
                forward(member, t + 2).start()

        @pl.when(t == 0)
        def _():
            for dest in (2, 3):
                all_of(0, dest).wait_recv()

        slot = lax.rem(t, 2)
        part_sum[slot] = dot_t(rows[lax.rem(t + 1, RING)], gate_up[...].reshape(2 * hid, width))
        half_out[t] = part_sum[slot, pl.ds(its_half, half)].astype(BF)
        x_one(t).start()

    def stage_b(t):
        slot = lax.rem(t, 2)
        x_one(t).wait_recv()
        sent = part_sum[slot, pl.ds(pl.multiple_of(my_half + its_fourth, fourth), fourth)]
        quarter_out[t] = (sent + half_in[t, pl.ds(its_fourth, fourth)].astype(F32)).astype(BF)
        x_two(t).start()
        kept = part_sum[slot, pl.ds(mine, fourth)]
        quarter[slot] = kept + half_in[t, pl.ds(my_fourth, fourth)].astype(F32)

    def stage_c(t):
        slot = lax.rem(t, 2)
        x_two(t).wait_recv()
        both = quarter[slot] + quarter_in[t].astype(F32)
        gate, up_val = both[:, 0:hid], both[:, hid : 2 * hid]
        hidden[t, pl.ds(mine, fourth)] = (gate / (1.0 + jnp.exp(-gate)) * up_val).astype(BF)
        for d in (2, 1, 3):
            x_hidden(d, t).start()

    def stage_e(t):
        @pl.when(t == 0)
        def _():
            for dest in (2, 3):
                all_of(1, dest).wait_recv()

        span = pl.ds(0, whole - fourth)
        remote(
            hidden.at[t, span], hidden.at[t, span], y_send.at[0], y_recv.at[t], twin
        ).wait_recv()
        down_now[...] = dot(hidden[t], down_w[...].reshape(hid, width))

        @pl.when(t == RING - 1)
        def _():
            down_own[...] = down_now[...]

        for member in (0, 2, 1, 3):
            span = pl.ds(member * CAP, CAP)

            @pl.when(jnp.logical_and(t >= 1, t < RING - 1))
            def _(member=member, span=span):
                sum_on(member, t).wait_recv()
                down_now[span] += sum_in[t - 1, span].astype(F32)

            @pl.when(t < RING - 1)
            def _(member=member, span=span):
                sum_out[t, span] = down_now[span].astype(BF)
                sum_on(member, t + 1).start()

    scale_rows(0)
    forward(0, 1).start()
    send_weights(len(pending))
    for copy in across:
        copy.wait_recv()
    for d in (1, 3, 2):
        spread[d].wait_recv()
        scales[d].wait_recv()
        scale_rows(d)
        forward(d, 1).start()
    stages = (stage_a, stage_b, stage_c, stage_e)

    def turn(t, carry):
        for lag in LAGS:
            @pl.when(jnp.logical_and(t >= lag, t < RING + lag))
            def _(lag=lag):
                stages[lag](t - lag)

        return carry

    lax.fori_loop(0, RING + 3, turn, 0)
    back = {}
    for member in (2, 3, 1, 0):
        span = pl.ds(member * CAP, CAP)
        sum_on(member, RING - 1).wait_recv()
        down_own[span] += sum_in[RING - 2, span].astype(F32)
        if member:
            back_out[span] = down_own[span].astype(BF)
            back[member] = remote(
                back_out.at[span], back_in.at[member], back_send.at[0], back_recv.at[member],
                first_axis(y, z, core, RING - member * stride),
            )
            back[member].start()
    mlp = down_own[0:CAP, :]
    for d in range(1, MEMBERS):
        back[d].wait_recv()
        mlp = mlp + back_in[d].astype(F32)
    mlp = mlp.astype(BF).astype(F32)
    result = x_rows + router * (attn[...] + mlp)
    out_ref[...] = jnp.where(live, result, 0.0).astype(BF)
    for copy in copies:
        copy.wait_send()
    for kind in range(2):
        for dest in (2, 3):
            all_of(kind, dest).wait_send()
    others = pl.ds(CAP, whole - CAP)
    for ref, sem in (
        (kv.at[0, 0, pl.ds(1, RING - 1)], near_send.at[0]),
        (kv.at[0, pl.ds(1, RING - 1)], far_send.at[0]),
        (kv.at[1], chip_send.at[0]),
        (squares.at[pl.ds(1, TP - 1)], sq_send.at[0]),
        (raw.at[pl.ds(1, MEMBERS - 1)], row_send.at[0]),
        (tiles.at[pl.ds(1, MEMBERS - 1)], tile_send.at[0]),
        (rows.at[pl.ds(1, RING - 1)], ring_send.at[0]),
        (sum_out, sum_send.at[0]),
        (half_out, x_send.at[0]),
        (quarter_out, x_send.at[1]),
        (hidden.at[:, pl.ds(0, whole - fourth)], y_send.at[0]),
        (back_out.at[others], back_send.at[0]),
    ):
        remote(ref, ref, sem, sem, twin).wait_send()


def vmem(count):
    return [pl.BlockSpec(memory_space=pltpu.VMEM)] * count


SCALAR = pl.BlockSpec(memory_space=pltpu.SMEM)
DMA = pltpu.SemaphoreType.DMA


def local(
    resid, query, key, value, router_logit, norm_gain, w_gate, w_up, w_down, sel_index, sel_count
):
    width = resid.shape[1]
    tall = width // key.shape[1] * CAP
    heads = key.shape[1] // HEAD_DIM
    units = w_down.shape[0]
    whole = MEMBERS * CAP
    hid = BLOCKS * units
    return pl.pallas_call(
        block_kernel,
        out_shape=jax.ShapeDtypeStruct((CAP, width), BF),
        in_specs=[pl.BlockSpec(memory_space=pl.ANY)] * 10 + [SCALAR],
        out_specs=vmem(1)[0],
        scratch_shapes=[
            pltpu.VMEM(resid.shape, BF),
            pltpu.VMEM(query.shape, BF),
            pltpu.VMEM(key.shape, BF),
            pltpu.VMEM(value.shape, BF),
            pltpu.VMEM((1, router_logit.shape[0]), F32),
            pltpu.VMEM(norm_gain.shape, BF),
            pltpu.VMEM(sel_index.shape, jnp.int32),
            DMA((10,)),
            pltpu.VMEM((2, RING, RING, CAP, 2 * key.shape[1]), BF),
            pltpu.VMEM((heads, tall + 16, HEAD_DIM), BF),
            pltpu.VMEM((heads, tall, 1), F32),
            pltpu.VMEM((heads, tall, 1), F32),
            pltpu.VMEM((heads, tall, HEAD_DIM), F32),
            pltpu.VMEM((TP, CAP, HEAD_DIM), F32),
            pltpu.VMEM((1, RING * CAP), F32),
            pltpu.VMEM((CAP, width), F32),
            pltpu.VMEM((2, BLOCKS, units, width), BF),
            pltpu.VMEM((BLOCKS, units, width), BF),
            pltpu.VMEM((RING, whole, width), BF),
            pltpu.VMEM((MEMBERS, CAP, width), BF),
            pltpu.VMEM((MEMBERS, CAP, HEAD_DIM), F32),
            pltpu.VMEM((2, whole, 2 * hid), F32),
            pltpu.VMEM((2, whole // 4, 2 * hid), F32),
            pltpu.VMEM((RING, whole // 2, 2 * hid), BF),
            pltpu.VMEM((RING, whole // 2, 2 * hid), BF),
            pltpu.VMEM((RING, whole // 4, 2 * hid), BF),
            pltpu.VMEM((RING, whole // 4, 2 * hid), BF),
            pltpu.VMEM((RING, whole, hid), BF),
            pltpu.VMEM((RING - 1, whole, width), BF),
            pltpu.VMEM((RING - 1, whole, width), BF),
            pltpu.VMEM((whole, width), F32),
            pltpu.VMEM((whole, width), F32),
            pltpu.VMEM((whole, width), BF),
            pltpu.VMEM((MEMBERS, CAP, width), BF),
            DMA((1,)), DMA((RING,)),
            DMA((1,)), DMA((RING - 1, RING)),
            DMA((1,)), DMA((RING,)),
            DMA((1,)), DMA((1,)),
            DMA((2, 3)), DMA((2, 3)),
            DMA((1,)), DMA((MEMBERS,)),
            DMA((1,)), DMA((MEMBERS,)),
            DMA((1,)), DMA((MEMBERS, RING)),
            DMA((2,)), DMA((2, RING)),
            DMA((1,)), DMA((RING,)),
            DMA((1,)), DMA((MEMBERS, RING)),
            DMA((1,)), DMA((MEMBERS,)),
        ],
        compiler_params=pltpu.CompilerParams(collective_id=0, has_side_effects=True),
        name="block",
    )(
        resid, query, key, value, router_logit[None, :], norm_gain, sel_index,
        w_gate.T, w_up.T, w_down, sel_count,
    )


def solution(mesh):
    split = Mesh(mesh.devices.reshape(8, 8, 2, mesh.shape["tp"]), (*CTX, "tp"))
    placed = (
        P(CTX, "tp"),
        P(CTX, "tp"),
        P(CTX, "tp"),
        P(CTX, "tp"),
        P(CTX),
        P("tp"),
        P("tp", CTX),
        P("tp", CTX),
        P(CTX, "tp"),
        P(CTX, None),
        P(CTX),
    )
    return jax.shard_map(
        local, mesh=split, in_specs=placed, out_specs=P(CTX, "tp"), check_vma=False
    )
```
